128 devices in a mesh: samples: 4 (over x, y), px: 16 (over z), py: 2 (over core).
Axes of the slice: x: 2, y: 2, z: 16, core: 2. Of those that a mesh axis runs over, the one named last changes fastest.
The devices are a block of a 8x8x16 slice.
Arguments:
- source: float32 [2, 1024, 256, 256], P(None, 'samples', 'px', 'py'), parts along dimension 1, may hold values from -6 to 6
- speed: float32 [1024, 256, 256], P('samples', 'px', 'py'), parts along dimension 0, may hold values from 0.5 to 3
Outputs:
- solution: float32 [2, 1024, 256, 256], P(None, 'samples', 'px', 'py'), parts along dimension 1
The draws below stay inside these ranges and needn't reach their ends.
There are 4 independent parts, one for each index of `samples`. The reference program is written for one: setup_inputs(seed, part) draws one part's arguments, and reference() takes and returns one part's arrays. A program takes and returns all parts, laid end to end along the dimension named above; each array names one. Nothing has to cross between parts.
All inputs are finite; a program needn't handle non-finite values.
Results may differ from the reference program's by a relative error of at most 0.00024.
Values sent between devices are 32-bit elements; how exact they have to be, the bound alone decides.
No kernel may reach another device: no remote copies, remote signals or barrier semaphores. Data moves between devices by JAX's collectives and lax.ppermute only.
A program may use at most 192 MiB of HBM per device.

```python
import math
import jax
import jax.numpy as jnp
from jax import lax

NX = 256
NY = 256
NZ = 256


def draw_source(key, part):
    normal_part = jnp.clip(jax.random.normal(key, (2, NX, NY, NZ), jnp.float32), -6.0, 6.0)
    return normal_part


def level_of(own_key, extent, shards, low, largest):
    loudness, own = 1.0, jax.random.fold_in(own_key, 6)
    for position, parts in shards:
        heights = jnp.exp(jax.random.uniform(jax.random.fold_in(own, position), (parts,), jnp.float32, low / len(shards), largest / len(shards)))
        loudness = loudness * jnp.repeat(heights, extent[position] // parts).reshape([-1 if axis == position else 1 for axis in range(len(extent))])
    return loudness


def setup_inputs(seed: int = 0, part: int = 0) -> dict:
    key_list = jax.random.split(jax.random.key(seed), 3)
    part_splits = jax.random.split(jax.random.fold_in(key_list[2], part), 3)
    return {
        "source": draw_source(jax.random.fold_in(jax.random.fold_in(key_list[2], part), 71), part),
        "speed": jnp.clip(jnp.exp(math.log(3.0) - 1.7917595 * jax.random.uniform(part_splits[1], (NX, NY, NZ), jnp.float32) ** level_of(part_splits[1], (NX, NY, NZ), ((1, 16), (2, 2)), -0.2, 0.2)), 0.5, 3.0),
    }


wave_square = 0.25
damping = 0.5
epsilon = 1e-06
highest = lax.Precision.HIGHEST

def sine_table(length):
    positions = jnp.arange(length, dtype=jnp.float32) + 1.0
    phases = jnp.pi * positions[:, None] * positions[None, :] / (length + 1.0)
    return jnp.sqrt(2.0 / (length + 1.0)) * jnp.sin(phases)

def eigen_line(length, offset, number):
    positions = jnp.arange(number, dtype=jnp.float32) + jnp.asarray(offset).astype(jnp.float32) + 1.0
    sine_half = jnp.sin(jnp.pi * positions / (2.0 * (length + 1.0)))
    return 4.0 * sine_half * sine_half

def divide(values, eigen_x, eigen_y, eigen_z):
    shifted = eigen_x[:, None, None] + eigen_y[None, :, None] + eigen_z[None, None, :] - wave_square
    damped = damping * wave_square
    modulus = shifted * shifted + damped * damped
    real_part = (values[0] * shifted + values[1] * damped) / modulus
    imag_part = (values[1] * shifted - values[0] * damped) / modulus
    return jnp.stack([real_part, imag_part])

def transform(values, matrix_x, matrix_y, matrix_z):
    values = jnp.einsum('ak,ckyz->cayz', matrix_x, values, precision=highest)
    values = jnp.einsum('ak,cxkz->cxaz', matrix_y, values, precision=highest)
    return jnp.einsum('ak,cxyk->cxya', matrix_z, values, precision=highest)

def precondition(vector):
    matrix_x = sine_table(NX)
    matrix_y = sine_table(NY)
    matrix_z = sine_table(NZ)
    spectral = transform(vector, matrix_x, matrix_y, matrix_z)
    scaled = divide(spectral, eigen_line(NX, 0, NX), eigen_line(NY, 0, NY), eigen_line(NZ, 0, NZ))
    return transform(scaled, matrix_x, matrix_y, matrix_z)

def operate(vector, wave_field):
    padded = jnp.pad(vector, ((0, 0), (1, 1), (1, 1), (1, 1)))
    neighbours = padded[:, 2:, 1:-1, 1:-1] + padded[:, :-2, 1:-1, 1:-1]
    neighbours = neighbours + padded[:, 1:-1, 2:, 1:-1] + padded[:, 1:-1, :-2, 1:-1]
    neighbours = neighbours + padded[:, 1:-1, 1:-1, 2:] + padded[:, 1:-1, 1:-1, :-2]
    return (6.0 - wave_field) * vector - neighbours

def inner_sums(left, right):
    real_sum = jnp.sum(left[0] * right[0] + left[1] * right[1])
    imag_sum = jnp.sum(left[0] * right[1] - left[1] * right[0])
    return (real_sum, imag_sum)

def scaled_by(factor, vector):
    real_part = factor[0] * vector[0] - factor[1] * vector[1]
    imag_part = factor[0] * vector[1] + factor[1] * vector[0]
    return jnp.stack([real_part, imag_part])

def reference(source, speed):
    wave_field = wave_square / (speed * speed)
    source_size = jnp.sqrt(jnp.sum(source * source) + epsilon)
    basis_one = source / source_size
    solved_one = precondition(basis_one)
    applied = operate(solved_one, wave_field)
    one_re, one_im = inner_sums(basis_one, applied)
    remainder = applied - scaled_by((one_re, one_im), basis_one)
    two_one = jnp.sqrt(jnp.sum(remainder * remainder) + epsilon)
    denominator = one_re * one_re + one_im * one_im + two_one * two_one
    weight = (source_size * one_re / denominator, -source_size * one_im / denominator)
    return scaled_by(weight, solved_one)
```

```python
import functools
import numpy as np
import jax
import jax.numpy as jnp
from jax import lax
from jax.experimental import pallas as pl
from jax.experimental.pallas import tpu as pltpu
from jax.sharding import PartitionSpec as P

wave_square = 0.25
damping = 0.5
epsilon = 1e-06
f32 = jnp.float32
bf16 = jnp.bfloat16
YB = 8
KB = 32


def sine_table(length):
    k = np.arange(1, length + 1, dtype=np.float64)
    phases = np.mod(np.outer(k, k), 2 * (length + 1)) * (np.pi / (length + 1))
    return np.sqrt(2.0 / (length + 1)) * np.sin(phases)


def halves_of(table):
    table = table.astype(np.float32)
    high = table.astype(bf16)
    low = (table - high.astype(np.float32)).astype(bf16)
    return high, low


def eigen_line(length):
    k = np.arange(1, length + 1, dtype=np.float64)
    return 4.0 * np.sin(np.pi * k / (2.0 * (length + 1))) ** 2


def root_tables(nx, nz):
    near = eigen_line(nx)[:, None] + eigen_line(nz)[None, :] - wave_square + 1j * damping * wave_square
    spread = np.sqrt(near) * np.sqrt(near + 4.0)
    lam = 2.0 / (near + 2.0 + spread)
    gam = 1.0 / spread
    return np.stack([lam.real, lam.imag, gam.real, gam.imag]).astype(np.float32)


def cmul(a, b):
    return a[0] * b[0] - a[1] * b[1], a[0] * b[1] + a[1] * b[0]


def cadd(a, b):
    return a[0] + b[0], a[1] + b[1]


def split(v):
    high = v.astype(bf16)
    return high, (v - high.astype(f32)).astype(bf16)


def dot(a, b):
    return lax.dot_general(a, b, (((1,), (0,)), ((), ())), preferred_element_type=f32)


def forward_x(s_ref, src, send, keep):
    me = lax.axis_index("py")
    nx = src.shape[1]
    flat = src.at[0].reshape(nx * YB, src.shape[3])
    cols = []
    for y in range(YB):
        high, low = split(flat[pl.ds(y, nx, stride=YB), :])
        cols.append(jnp.concatenate([high, low, high], axis=0))
    right = jnp.concatenate(cols, axis=1)
    for half, out in ((1 - me, send), (me, keep)):
        got = dot(s_ref[half], right)
        w = src.shape[3]
        for y in range(YB):
            out[0, y] = got[:, y * w : (y + 1) * w]


def forward_z(s_ref, root, keep, recv, f_out, pq):
    me = lax.axis_index("py")
    _, ny, kb, w = keep.shape
    total = None
    for half, ref in ((me, keep), (1 - me, recv)):
        high, low = split(ref[...].reshape(2 * ny * kb, w))
        part = dot(jnp.concatenate([high, low, high], axis=1), s_ref[half])
        total = part if total is None else total + part
    f_out[...] = total.reshape(f_out.shape)
    nk = root.shape[1] // 2
    rows = pl.ds(pl.multiple_of(me * nk + pl.program_id(0) * kb, kb), kb)
    lam = root[0, rows, :], root[1, rows, :]
    p = f_out[0, 0], f_out[1, 0]
    q = f_out[0, ny - 1], f_out[1, ny - 1]
    for j in range(1, ny):
        p = cadd(cmul(lam, p), (f_out[0, j], f_out[1, j]))
        q = cadd(cmul(lam, q), (f_out[0, ny - 1 - j], f_out[1, ny - 1 - j]))
    for i, part in enumerate((*p, *q)):
        pq[:, i] = part.reshape(pq.shape[0], pq.shape[2], pq.shape[3])


def local_solve(root, f_ref, w_out):
    me = lax.axis_index("py")
    _, ny, kb, _ = f_ref.shape
    nk = root.shape[1] // 2
    rows = pl.ds(pl.multiple_of(me * nk + pl.program_id(0) * kb, kb), kb)
    lam = root[0, rows, :], root[1, rows, :]
    gam = root[2, rows, :], root[3, rows, :]
    p = None
    for j in range(ny):
        f = f_ref[0, j], f_ref[1, j]
        p = f if p is None else cadd(cmul(lam, p), f)
        w_out[0, j], w_out[1, j] = p
    q = None
    for j in reversed(range(ny)):
        lq = None if q is None else cmul(lam, q)
        here = w_out[0, j], w_out[1, j]
        if lq is not None:
            here = cadd(here, lq)
            q = cadd(lq, (f_ref[0, j], f_ref[1, j]))
        else:
            q = f_ref[0, j], f_ref[1, j]
        w_out[0, j], w_out[1, j] = cmul(gam, here)


def carries(root, pq, fb):
    n, _, rows, _ = pq.shape
    first = (lax.axis_index("py") * n + lax.axis_index("px")) * rows
    own = pl.ds(pl.multiple_of(first, rows), rows)
    lam = root[0, own, :], root[1, own, :]
    gam = root[2, own, :], root[3, own, :]

    def power(base, exponent):
        result = None
        while exponent:
            if exponent & 1:
                result = base if result is None else cmul(result, base)
            exponent >>= 1
            if exponent:
                base = cmul(base, base)
        return result

    return lam, gam, power


def reduced_solve(ny, root, pq, fb):
    n = pq.shape[0]
    lam, gam, power = carries(root, pq, fb)
    block = power(lam, ny)
    whole = power(block, n)
    last_f = pq[0, 0], pq[0, 1]
    last_b = pq[n - 1, 2], pq[n - 1, 3]
    for i in range(1, n):
        last_f = cadd(cmul(block, last_f), (pq[i, 0], pq[i, 1]))
        last_b = cadd(cmul(block, last_b), (pq[n - 1 - i, 2], pq[n - 1 - i, 3]))
    around = cmul(whole, cmul(lam, lam))
    both = cmul(around, whole)
    det = 1.0 - both[0], -both[1]
    size = det[0] * det[0] + det[1] * det[1]
    inverse = det[0] / size, -det[1] / size
    minus = -lam[0], -lam[1]
    f = cmul(inverse, cadd(cmul(minus, last_b), cmul(around, last_f)))
    b = cmul(inverse, cadd(cmul(minus, last_f), cmul(around, last_b)))
    for i in range(n):
        fb[i, 0], fb[i, 1] = cmul(gam, f)
        k = n - 1 - i
        fb[k, 2], fb[k, 3] = cmul(gam, b)
        if i < n - 1:
            f = cadd(cmul(block, f), (pq[i, 0], pq[i, 1]))
            b = cadd(cmul(block, b), (pq[k, 2], pq[k, 3]))


def inverse_z(s_ref, root, w_ref, fb, send, keep, u):
    me = lax.axis_index("py")
    _, ny, kb, nz = w_ref.shape
    nk = root.shape[1] // 2
    rows = pl.ds(pl.multiple_of(me * nk + pl.program_id(0) * kb, kb), kb)
    lam = root[0, rows, :], root[1, rows, :]
    f = fb[:, 0].reshape(kb, nz), fb[:, 1].reshape(kb, nz)
    b = fb[:, 2].reshape(kb, nz), fb[:, 3].reshape(kb, nz)
    for j in range(ny):
        f = cmul(lam, f)
        u[0, j], u[1, j] = cadd((w_ref[0, j], w_ref[1, j]), f)
    for j in reversed(range(ny)):
        b = cmul(lam, b)
        u[0, j], u[1, j] = cadd((u[0, j], u[1, j]), b)
    high, low = split(u[...].reshape(2 * ny * kb, nz))
    left = jnp.concatenate([high, low, high], axis=1)
    got = dot(left, jnp.concatenate([s_ref[1 - me], s_ref[me]], axis=1))
    w = send.shape[3]
    send[...] = got[:, :w].reshape(send.shape)
    keep[...] = got[:, w:].reshape(keep.shape)


def inverse_x(s_ref, keep, recv, src, speed, out, sums):
    me = lax.axis_index("py")
    _, nx, _, w = out.shape
    left = jnp.concatenate([s_ref[me], s_ref[1 - me]], axis=1)
    for c in range(2):
        cols = []
        for y in range(YB):
            parts = []
            for ref in (keep, recv):
                high, low = split(ref[c, y])
                parts += [high, low, high]
            cols.append(jnp.concatenate(parts, axis=0))
        got = dot(left, jnp.concatenate(cols, axis=1))
        flat = out.at[c].reshape(nx * YB, w)
        for y in range(YB):
            flat[pl.ds(y, nx, stride=YB), :] = got[:, y * w : (y + 1) * w]

    @pl.when(pl.program_id(0) == 0)
    def _():
        sums[...] = jnp.zeros_like(sums)

    damped = damping * wave_square

    def step(i, acc):
        s0, s1 = src[0, i], src[1, i]
        p0, p1 = out[0, i], out[1, i]
        c = speed[i]
        factor = wave_square - wave_square / (c * c)
        a0 = s0 + factor * p0 + damped * p1
        a1 = s1 + factor * p1 - damped * p0
        new = (
            s0 * s0 + s1 * s1,
            s0 * a0 + s1 * a1,
            s0 * a1 - s1 * a0,
            a0 * a0 + a1 * a1,
        )
        return tuple(x + y for x, y in zip(acc, new))

    zero = jnp.zeros((YB, w), f32)
    acc = lax.fori_loop(0, nx, step, (zero,) * 4, unroll=8)
    for i, a in enumerate(acc):
        sums[i : i + 1, :] += jnp.sum(a, axis=0, keepdims=True)


def finish(total, ps, out):
    sums = jnp.sum(jnp.sum(total[...], axis=0), axis=1, keepdims=True)
    square, re, im, size = (sums[i : i + 1] for i in range(4))
    beta2 = square + epsilon
    re, im, size = re / beta2, im / beta2, size / beta2
    den = size - (re * re + im * im) * (epsilon / beta2) + epsilon
    a, b = re / den, -im / den
    shape = ps.shape[1:]
    a = jnp.broadcast_to(a[:, :, None], shape)
    b = jnp.broadcast_to(b[:, :, None], shape)
    out[0] = a * ps[0] - b * ps[1]
    out[1] = a * ps[1] + b * ps[0]


def params(parallel=1):
    return pltpu.CompilerParams(dimension_semantics=("arbitrary",) * parallel, vmem_limit_bytes=56 * 2**20)


def whole(a):
    return pl.BlockSpec(a.shape, lambda *_: (0,) * a.ndim)


def cost(flops, moved):
    return pl.CostEstimate(flops=flops, bytes_accessed=moved, transcendentals=0)


def on_device(source, speed):
    _, nx, ny, w = source.shape
    cores, ring = lax.axis_size("py"), lax.axis_size("px")
    nz, nk = w * cores, nx // cores
    other = [(i, cores - 1 - i) for i in range(cores)]
    sds = lambda *shape: jax.ShapeDtypeStruct(shape, f32)

    hx, lx = halves_of(sine_table(nx))
    hz, lz = halves_of(sine_table(nz))
    sx_in = jnp.asarray(np.concatenate([hx, hx, lx], 1).reshape(2, nk, 3 * nx))
    sz_in = jnp.asarray(np.stack([np.concatenate([hz[h * w : (h + 1) * w]] * 2 + [lz[h * w : (h + 1) * w]], 0) for h in (0, 1)]))
    sz_out = jnp.asarray(np.stack([np.concatenate([hz, hz, lz], 0)[:, h * w : (h + 1) * w] for h in (0, 1)]))
    sx_out = jnp.asarray(np.stack([np.concatenate([t[:, h * nk : (h + 1) * nk] for t in (hx, hx, lx)], 1) for h in (0, 1)]))
    root = jnp.asarray(root_tables(nx, nz))
    part = sds(2, ny, nk, w)
    flops = 2 * 2 * nx * ny * w * nx * 3

    spec = pl.BlockSpec((1, YB, nk, w), lambda c, y: (c, y, 0, 0))
    send, keep = pl.pallas_call(
        forward_x,
        grid=(2, ny // YB),
        in_specs=[whole(sx_in), pl.BlockSpec((1, nx, YB, w), lambda c, y: (c, 0, y, 0))],
        out_specs=[spec, spec],
        out_shape=[part, part],
        compiler_params=params(2),
        cost_estimate=cost(flops, 8 * 2**20),
        name="forward_x",
    )(sx_in, source)
    recv = lax.ppermute(send, "py", other)

    kspec = lambda width: pl.BlockSpec((2, ny, KB, width), lambda k: (0, 0, k, 0))
    rows = nk // ring
    pspec = pl.BlockSpec((KB // rows, 4, rows, nz), lambda k: (k, 0, 0, 0))
    f, pq = pl.pallas_call(
        forward_z,
        grid=(nk // KB,),
        in_specs=[whole(sz_in), whole(root), kspec(w), kspec(w)],
        out_specs=[kspec(nz), pspec],
        out_shape=[sds(2, ny, nk, nz), sds(ring, 4, rows, nz)],
        compiler_params=params(),
        cost_estimate=cost(flops, 8 * 2**20),
        name="forward_z",
    )(sz_in, root, keep, recv)
    pq = lax.all_to_all(pq, "px", 0, 0, tiled=True)
    local = pl.pallas_call(
        local_solve,
        grid=(nk // KB,),
        in_specs=[whole(root), kspec(nz)],
        out_specs=kspec(nz),
        out_shape=sds(2, ny, nk, nz),
        compiler_params=params(),
        cost_estimate=cost(flops, 8 * 2**20),
        name="local_solve",
    )(root, f)
    fb = pl.pallas_call(
        functools.partial(reduced_solve, ny),
        out_shape=sds(ring, 4, rows, nz),
        compiler_params=pltpu.CompilerParams(vmem_limit_bytes=16 * 2**20),
        cost_estimate=cost(10**7, 2**20),
        name="reduced_solve",
    )(root, pq)
    fb = lax.all_to_all(fb, "px", 0, 0, tiled=True)
    send, keep = pl.pallas_call(
        inverse_z,
        grid=(nk // KB,),
        in_specs=[whole(sz_out), whole(root), kspec(nz), pspec],
        out_specs=[kspec(w), kspec(w)],
        out_shape=[part, part],
        scratch_shapes=[pltpu.VMEM((2, ny, KB, nz), f32)],
        compiler_params=params(),
        cost_estimate=cost(flops, 8 * 2**20),
        name="inverse_z",
    )(sz_out, root, local, fb)
    recv = lax.ppermute(send, "py", other)
    yspec = pl.BlockSpec((2, YB, nk, w), lambda y: (0, y, 0, 0))
    block = pl.BlockSpec((2, nx, YB, w), lambda y: (0, 0, y, 0))
    solved, sums = pl.pallas_call(
        inverse_x,
        grid=(ny // YB,),
        in_specs=[whole(sx_out), yspec, yspec, block, pl.BlockSpec((nx, YB, w), lambda y: (0, y, 0))],
        out_specs=[block, pl.BlockSpec((4, w), lambda y: (0, 0))],
        out_shape=[sds(*source.shape), sds(4, w)],
        compiler_params=params(),
        cost_estimate=cost(flops, 16 * 2**20),
        name="inverse_x",
    )(sx_out, keep, recv, source, speed)
    sums = sums + lax.ppermute(sums, "py", other)
    every = lax.all_to_all(jnp.broadcast_to(sums[None], (ring, 4, w)), "px", 0, 0, tiled=True)
    xb = nx // 8
    xspec = pl.BlockSpec((2, xb, ny, w), lambda x: (0, x, 0, 0))
    return pl.pallas_call(
        finish,
        grid=(nx // xb,),
        in_specs=[whole(every), xspec],
        out_specs=xspec,
        out_shape=sds(*source.shape),
        compiler_params=params(),
        cost_estimate=cost(10**7, 8 * 2**20),
        name="finish",
    )(every, solved)


def solution(mesh):
    return jax.shard_map(
        on_device,
        mesh=mesh,
        in_specs=(P(None, "samples", "px", "py"), P("samples", "px", "py")),
        out_specs=P(None, "samples", "px", "py"),
        check_vma=False,
    )
```

```python
import functools
import numpy as np
import jax
import jax.numpy as jnp
from jax import lax
from jax.experimental import pallas as pl
from jax.experimental.pallas import tpu as pltpu
from jax.sharding import PartitionSpec as P

wave_square = 0.25
damping = 0.5
epsilon = 1e-06
f32 = jnp.float32
bf16 = jnp.bfloat16
YB = 8
KB = 32
XC = 32


def sine_table(length):
    k = np.arange(1, length + 1, dtype=np.float64)
    phases = np.mod(np.outer(k, k), 2 * (length + 1)) * (np.pi / (length + 1))
    return np.sqrt(2.0 / (length + 1)) * np.sin(phases)


def halves_of(table):
    table = table.astype(np.float32)
    high = table.astype(bf16)
    low = (table - high.astype(np.float32)).astype(bf16)
    return high, low


def eigen_line(length):
    k = np.arange(1, length + 1, dtype=np.float64)
    return 4.0 * np.sin(np.pi * k / (2.0 * (length + 1))) ** 2


def root_tables(nx, nz):
    near = eigen_line(nx)[:, None] + eigen_line(nz)[None, :] - wave_square + 1j * damping * wave_square
    spread = np.sqrt(near) * np.sqrt(near + 4.0)
    lam = 2.0 / (near + 2.0 + spread)
    gam = 1.0 / spread
    return np.stack([lam.real, lam.imag, gam.real, gam.imag]).astype(np.float32)


def cmul(a, b):
    return a[0] * b[0] - a[1] * b[1], a[0] * b[1] + a[1] * b[0]


def cadd(a, b):
    return a[0] + b[0], a[1] + b[1]


def split(v):
    high = v.astype(bf16)
    return high, (v - high.astype(f32)).astype(bf16)


def dot(a, b):
    return lax.dot_general(a, b, (((1,), (0,)), ((), ())), preferred_element_type=f32)


def forward_x(s_ref, src, send, keep):
    me = lax.axis_index("py")
    nx = src.shape[1]
    flat = src.at[0].reshape(nx * YB, src.shape[3])
    cols = []
    for y in range(YB):
        high, low = split(flat[pl.ds(y, nx, stride=YB), :])
        cols.append(jnp.concatenate([high, low, high], axis=0))
    right = jnp.concatenate(cols, axis=1)
    for half, out in ((1 - me, send), (me, keep)):
        got = dot(s_ref[half], right)
        w = src.shape[3]
        for y in range(YB):
            out[0, y] = got[:, y * w : (y + 1) * w]


def own_rows(root, block, kb):
    nk = root.shape[1] // 2
    return pl.ds(pl.multiple_of(lax.axis_index("py") * nk + block * kb, kb), kb)


def power(base, exponent):
    result = None
    while exponent:
        if exponent & 1:
            result = base if result is None else cmul(result, base)
        exponent >>= 1
        if exponent:
            base = cmul(base, base)
    return result


def forward_z(first, s_ref, root, *refs):
    if first:
        keep, recv, f_out, pq = refs
    else:
        keep, recv, before, f_out, pq = refs
    me = lax.axis_index("py")
    _, ny, nk, w = keep.shape
    nz = f_out.shape[3]

    def block(i, carry):
        k = pl.ds(pl.multiple_of(i * KB, KB), KB)
        total = None
        for half, ref in ((me, keep), (1 - me, recv)):
            high, low = split(ref[:, :, k, :].reshape(2 * ny * KB, w))
            part = dot(jnp.concatenate([high, low, high], axis=1), s_ref[half])
            total = part if total is None else total + part
        total = total.reshape(2, ny, KB, nz)
        f_out[:, :, k, :] = total
        rows = own_rows(root, i, KB)
        lam = root[0, rows, :], root[1, rows, :]
        row = [(total[0, j], total[1, j]) for j in range(ny)]
        p = row[0] if first else cadd(cmul(lam, (before[0, k, :], before[1, k, :])), row[0])
        q = row[ny - 1]
        for j in range(1, ny):
            p = cadd(cmul(lam, p), row[j])
            q = cadd(cmul(lam, q), row[ny - 1 - j])
        if first:
            for c, part in enumerate((*p, *q)):
                pq[c, k, :] = part
        else:
            q = cadd(cmul(power(lam, ny), q), (before[2, k, :], before[3, k, :]))
            step = pq.shape[2]
            for c, part in enumerate((*p, *q)):
                pq[pl.ds(i * (KB // step), KB // step), c] = part.reshape(KB // step, step, nz)
        return carry

    lax.fori_loop(0, nk // KB, block, 0)


def local_solve(root, f0, f1, w0, w1):
    _, half, nk, _ = f0.shape
    ny = 2 * half

    def row(refs, j, k):
        ref = refs[j // half]
        return ref[0, j % half, k, :], ref[1, j % half, k, :]

    def block(i, carry):
        k = pl.ds(pl.multiple_of(i * KB, KB), KB)
        rows = own_rows(root, i, KB)
        lam = root[0, rows, :], root[1, rows, :]
        gam = root[2, rows, :], root[3, rows, :]

        def put(j, value):
            ref = (w0, w1)[j // half]
            ref[0, j % half, k, :], ref[1, j % half, k, :] = value

        p = None
        for j in range(ny):
            f = row((f0, f1), j, k)
            p = f if p is None else cadd(cmul(lam, p), f)
            put(j, p)
        q = None
        for j in reversed(range(ny)):
            here = row((w0, w1), j, k)
            if q is None:
                q = row((f0, f1), j, k)
            else:
                q = cmul(lam, q)
                here = cadd(here, q)
                q = cadd(q, row((f0, f1), j, k))
            put(j, cmul(gam, here))
        return carry

    lax.fori_loop(0, nk // KB, block, 0)


def reduced_solve(ny, root, pq, fb):
    n, _, rows, _ = pq.shape
    first = (lax.axis_index("py") * n + lax.axis_index("px")) * rows
    own = pl.ds(pl.multiple_of(first, rows), rows)
    lam = root[0, own, :], root[1, own, :]
    gam = root[2, own, :], root[3, own, :]
    block = power(lam, ny)
    whole = power(block, n)
    last_f = pq[0, 0], pq[0, 1]
    last_b = pq[n - 1, 2], pq[n - 1, 3]
    for i in range(1, n):
        last_f = cadd(cmul(block, last_f), (pq[i, 0], pq[i, 1]))
        last_b = cadd(cmul(block, last_b), (pq[n - 1 - i, 2], pq[n - 1 - i, 3]))
    around = cmul(whole, cmul(lam, lam))
    both = cmul(around, whole)
    det = 1.0 - both[0], -both[1]
    size = det[0] * det[0] + det[1] * det[1]
    inverse = det[0] / size, -det[1] / size
    minus = -lam[0], -lam[1]
    f = cmul(inverse, cadd(cmul(minus, last_b), cmul(around, last_f)))
    b = cmul(inverse, cadd(cmul(minus, last_f), cmul(around, last_b)))
    for i in range(n):
        fb[i, 0], fb[i, 1] = cmul(gam, f)
        k = n - 1 - i
        fb[k, 2], fb[k, 3] = cmul(gam, b)
        if i < n - 1:
            f = cadd(cmul(block, f), (pq[i, 0], pq[i, 1]))
            b = cadd(cmul(block, b), (pq[k, 2], pq[k, 3]))


def inverse_z(part, s_ref, root, w_ref, fb, send, keep, u):
    me = lax.axis_index("py")
    _, ny, nk, nz = w_ref.shape
    w = send.shape[3]

    def block(i, carry):
        k = pl.ds(pl.multiple_of(i * KB, KB), KB)
        rows = own_rows(root, i, KB)
        lam = root[0, rows, :], root[1, rows, :]
        step = fb.shape[2]
        got = pl.ds(i * (KB // step), KB // step)
        f = fb[got, 0].reshape(KB, nz), fb[got, 1].reshape(KB, nz)
        b = fb[got, 2].reshape(KB, nz), fb[got, 3].reshape(KB, nz)
        past = power(lam, ny)
        if part:
            f = cmul(past, f)
        else:
            b = cmul(past, b)
        for j in range(ny):
            f = cmul(lam, f)
            u[0, j], u[1, j] = cadd((w_ref[0, j, k, :], w_ref[1, j, k, :]), f)
        for j in reversed(range(ny)):
            b = cmul(lam, b)
            u[0, j], u[1, j] = cadd((u[0, j], u[1, j]), b)
        high, low = split(u[...].reshape(2 * ny * KB, nz))
        left = jnp.concatenate([high, low, high], axis=1)
        out = dot(left, jnp.concatenate([s_ref[1 - me], s_ref[me]], axis=1))
        send[:, :, k, :] = out[:, :w].reshape(2, ny, KB, w)
        keep[:, :, k, :] = out[:, w:].reshape(2, ny, KB, w)
        return carry

    lax.fori_loop(0, nk // KB, block, 0)


def inverse_x(part, s_ref, keep, recv, src_hbm, speed_hbm, out, sums, src, speed, sems):
    me = lax.axis_index("py")
    _, nx, _, w = out.shape
    rows = pl.ds(part * YB, YB)
    copies = [
        pltpu.make_async_copy(src_hbm.at[:, :, rows, :], src, sems.at[0]),
        pltpu.make_async_copy(speed_hbm.at[:, rows, :], speed, sems.at[1]),
    ]
    for copy in copies:
        copy.start()
    left = jnp.concatenate([s_ref[me], s_ref[1 - me]], axis=1)
    for c in range(2):
        cols = []
        for y in range(YB):
            parts = []
            for ref in (keep, recv):
                high, low = split(ref[c, y])
                parts += [high, low, high]
            cols.append(jnp.concatenate(parts, axis=0))
        got = dot(left, jnp.concatenate(cols, axis=1))
        flat = out.at[c].reshape(nx * YB, w)
        for y in range(YB):
            flat[pl.ds(y, nx, stride=YB), :] = got[:, y * w : (y + 1) * w]
    for copy in copies:
        copy.wait()
    damped = damping * wave_square

    def step(i, acc):
        s0, s1 = src[0, i], src[1, i]
        p0, p1 = out[0, i], out[1, i]
        c = speed[i]
        factor = wave_square - wave_square / (c * c)
        a0 = s0 + factor * p0 + damped * p1
        a1 = s1 + factor * p1 - damped * p0
        new = (
            s0 * s0 + s1 * s1,
            s0 * a0 + s1 * a1,
            s0 * a1 - s1 * a0,
            a0 * a0 + a1 * a1,
        )
        return tuple(x + y for x, y in zip(acc, new))

    zero = jnp.zeros((YB, w), f32)
    acc = lax.fori_loop(0, nx, step, (zero,) * 4, unroll=8)
    for i, a in enumerate(acc):
        sums[i : i + 1, :] = jnp.sum(a, axis=0, keepdims=True)


def finish(total, ps0, ps1, out_hbm, scaled, sems):
    sums = jnp.sum(jnp.sum(total[...], axis=0), axis=1, keepdims=True)
    square, re, im, size = (sums[i : i + 1] for i in range(4))
    beta2 = square + epsilon
    re, im, size = re / beta2, im / beta2, size / beta2
    den = size - (re * re + im * im) * (epsilon / beta2) + epsilon
    a, b = re / den, -im / den
    _, nx, _, w = ps0.shape
    a = jnp.broadcast_to(a, (YB, w))
    b = jnp.broadcast_to(b, (YB, w))
    copies = []
    for part, ps in enumerate((ps0, ps1)):
        for x in range(0, nx, XC):
            for i in range(x, x + XC):
                p0, p1 = ps[0, i], ps[1, i]
                scaled[part, 0, i] = a * p0 - b * p1
                scaled[part, 1, i] = a * p1 + b * p0
            copy = pltpu.make_async_copy(
                scaled.at[part, :, pl.ds(x, XC)],
                out_hbm.at[:, pl.ds(x, XC), pl.ds(part * YB, YB), :],
                sems.at[len(copies)],
            )
            copy.start()
            copies.append(copy)
    for copy in copies:
        copy.wait()


def params(mib, *dims):
    return pltpu.CompilerParams(dimension_semantics=dims or None, vmem_limit_bytes=mib * 2**20)


def whole(a):
    return pl.BlockSpec(a.shape, lambda *_: (0,) * a.ndim)


VM = pl.BlockSpec(memory_space=pltpu.VMEM)
ANY = pl.BlockSpec(memory_space=pl.ANY)


def cost(flops, moved):
    return pl.CostEstimate(flops=flops, bytes_accessed=moved, transcendentals=0)


def on_device(source, speed):
    _, nx, ny, w = source.shape
    cores, ring = lax.axis_size("py"), lax.axis_size("px")
    nz, nk = w * cores, nx // cores
    other = [(i, cores - 1 - i) for i in range(cores)]
    sds = lambda *shape: jax.ShapeDtypeStruct(shape, f32)

    hx, lx = halves_of(sine_table(nx))
    hz, lz = halves_of(sine_table(nz))
    sx_in = jnp.asarray(np.concatenate([hx, hx, lx], 1).reshape(2, nk, 3 * nx))
    sz_in = jnp.asarray(np.stack([np.concatenate([hz[h * w : (h + 1) * w]] * 2 + [lz[h * w : (h + 1) * w]], 0) for h in (0, 1)]))
    sz_out = jnp.asarray(np.stack([np.concatenate([hz, hz, lz], 0)[:, h * w : (h + 1) * w] for h in (0, 1)]))
    sx_out = jnp.asarray(np.stack([np.concatenate([t[:, h * nk : (h + 1) * nk] for t in (hx, hx, lx)], 1) for h in (0, 1)]))
    root = jnp.asarray(root_tables(nx, nz))
    piece = sds(2, YB, nk, w)
    modes = sds(2, YB, nk, nz)
    rows = nk // ring
    flops = 2 * 2 * nx * YB * w * nx * 3
    est = cost(flops, 4 * 2**20)

    spec = pl.BlockSpec((1, YB, nk, w), lambda c: (c, 0, 0, 0))
    moved = []
    for h in range(2):
        send, keep = pl.pallas_call(
            forward_x,
            grid=(2,),
            in_specs=[whole(sx_in), pl.BlockSpec((1, nx, YB, w), functools.partial(lambda h, c: (c, 0, h, 0), h))],
            out_specs=[spec, spec],
            out_shape=[piece, piece],
            compiler_params=params(12, "arbitrary"),
            cost_estimate=est,
            name="forward_x",
        )(sx_in, source)
        moved.append((keep, lax.ppermute(send, "py", other)))
    f, carry = [], ()
    for h in range(2):
        got, pq = pl.pallas_call(
            functools.partial(forward_z, h == 0),
            in_specs=[VM] * (4 + len(carry)),
            out_specs=[VM, VM],
            out_shape=[modes, sds(4, nk, nz) if h == 0 else sds(ring, 4, rows, nz)],
            compiler_params=params(12),
            cost_estimate=est,
            name="forward_z",
        )(sz_in, root, *moved[h], *carry)
        f.append(got)
        carry = (pq,)
    pq = lax.all_to_all(pq, "px", 0, 0, tiled=True)
    local = pl.pallas_call(
        local_solve,
        in_specs=[VM] * 3,
        out_specs=[VM, VM],
        out_shape=[modes, modes],
        compiler_params=params(8),
        cost_estimate=cost(2 * flops, 8 * 2**20),
        name="local_solve",
    )(root, *f)
    fb = pl.pallas_call(
        functools.partial(reduced_solve, ny),
        in_specs=[VM] * 2,
        out_specs=VM,
        out_shape=sds(ring, 4, rows, nz),
        compiler_params=params(8),
        cost_estimate=cost(10**7, 2**20),
        name="reduced_solve",
    )(root, pq)
    fb = lax.all_to_all(fb, "px", 0, 0, tiled=True)
    moved = []
    for h in range(2):
        send, keep = pl.pallas_call(
            functools.partial(inverse_z, h),
            in_specs=[VM] * 4,
            out_specs=[VM, VM],
            out_shape=[piece, piece],
            scratch_shapes=[pltpu.VMEM((2, YB, KB, nz), f32)],
            compiler_params=params(12),
            cost_estimate=est,
            name="inverse_z",
        )(sz_out, root, local[h], fb)
        moved.append((keep, lax.ppermute(send, "py", other)))
    solved, sums = [], []
    for h in range(2):
        got, part = pl.pallas_call(
            functools.partial(inverse_x, h),
            in_specs=[VM, VM, VM, ANY, ANY],
            out_specs=[VM, VM],
            out_shape=[sds(2, nx, YB, w), sds(4, w)],
            scratch_shapes=[pltpu.VMEM((2, nx, YB, w), f32), pltpu.VMEM((nx, YB, w), f32), pltpu.SemaphoreType.DMA((2,))],
            compiler_params=params(16),
            cost_estimate=est,
            name="inverse_x",
        )(sx_out, *moved[h], source, speed)
        solved.append(got)
        sums.append(part)
    sums = sums[0] + sums[1]
    sums = sums + lax.ppermute(sums, "py", other)
    every = lax.all_to_all(jnp.broadcast_to(sums[None], (ring, 4, w)), "px", 0, 0, tiled=True)
    return pl.pallas_call(
        finish,
        in_specs=[VM] * 3,
        out_specs=ANY,
        out_shape=sds(*source.shape),
        scratch_shapes=[pltpu.VMEM((2, 2, nx, YB, w), f32), pltpu.SemaphoreType.DMA((2 * nx // XC,))],
        compiler_params=params(16),
        cost_estimate=cost(10**7, 8 * 2**20),
        name="finish",
    )(every, *solved)


def solution(mesh):
    return jax.shard_map(
        on_device,
        mesh=mesh,
        in_specs=(P(None, "samples", "px", "py"), P("samples", "px", "py")),
        out_specs=P(None, "samples", "px", "py"),
        check_vma=False,
    )
```

```python
import functools
import numpy as np
import jax
import jax.numpy as jnp
from jax import lax
from jax.experimental import pallas as pl
from jax.experimental.pallas import tpu as pltpu
from jax.sharding import PartitionSpec as P

wave_square = 0.25
damping = 0.5
epsilon = 1e-06
f32 = jnp.float32
bf16 = jnp.bfloat16
YB = 8
KB = 32
XC = 32
CHUNKS = 2


def sine_table(length):
    k = np.arange(1, length + 1, dtype=np.float64)
    phases = np.mod(np.outer(k, k), 2 * (length + 1)) * (np.pi / (length + 1))
    return np.sqrt(2.0 / (length + 1)) * np.sin(phases)


def halves_of(table):
    table = table.astype(np.float32)
    high = table.astype(bf16)
    low = (table - high.astype(np.float32)).astype(bf16)
    return high, low


def eigen_line(length):
    k = np.arange(1, length + 1, dtype=np.float64)
    return 4.0 * np.sin(np.pi * k / (2.0 * (length + 1))) ** 2


def root_tables(nx, nz):
    near = eigen_line(nx)[:, None] + eigen_line(nz)[None, :] - wave_square + 1j * damping * wave_square
    spread = np.sqrt(near) * np.sqrt(near + 4.0)
    lam = 2.0 / (near + 2.0 + spread)
    gam = 1.0 / spread
    return np.stack([lam.real, lam.imag, gam.real, gam.imag]).astype(np.float32)


def cmul(a, b):
    return a[0] * b[0] - a[1] * b[1], a[0] * b[1] + a[1] * b[0]


def cadd(a, b):
    return a[0] + b[0], a[1] + b[1]


def split(v):
    high = v.astype(bf16)
    return high, (v - high.astype(f32)).astype(bf16)


def dot(a, b):
    return lax.dot_general(a, b, (((1,), (0,)), ((), ())), preferred_element_type=f32)


def stack(s_ref, axis):
    return jnp.concatenate([s_ref[0], s_ref[0], s_ref[1]], axis=axis)


def by_half(me, keep, recv):
    first = me == 0
    return jnp.where(first, keep, recv), jnp.where(first, recv, keep)


def forward_x(part, s_ref, src, send, keep):
    me = lax.axis_index("py")
    _, nx, ny, w = src.shape
    nk = nx // 2
    for c in range(2):
        flat = src.at[c].reshape(nx * ny, w)
        cols = []
        for y in range(YB):
            high, low = split(flat[pl.ds(part * YB + y, nx, stride=ny), :])
            cols.append(jnp.concatenate([high, low, high], axis=0))
        right = jnp.concatenate(cols, axis=1)
        for half, out in ((1 - me, send), (me, keep)):
            rows = pl.ds(pl.multiple_of(half * nk, nk), nk)
            high, low = s_ref[0, rows, :], s_ref[1, rows, :]
            got = dot(jnp.concatenate([high, high, low], axis=1), right)
            for y in range(YB):
                out[c, y] = got[:, y * w : (y + 1) * w]


def own_rows(root, block, kb):
    nk = root.shape[1] // 2
    return pl.ds(pl.multiple_of(lax.axis_index("py") * nk + block * kb, kb), kb)


def power(base, exponent):
    result = None
    while exponent:
        if exponent & 1:
            result = base if result is None else cmul(result, base)
        exponent >>= 1
        if exponent:
            base = cmul(base, base)
    return result


def forward_z(first, s_ref, root, *refs):
    if first:
        keep, recv, f_out, pq = refs
    else:
        keep, recv, before, f_out, pq, *sends = refs
    me = lax.axis_index("py")
    ring, place = lax.axis_size("px"), lax.axis_index("px")
    _, ny, nk, w = keep.shape
    nz = f_out.shape[3]

    def block(send, base, i):
        k = pl.ds(pl.multiple_of((base + i) * KB, KB), KB)
        shape = 2 * ny * KB, w
        both = by_half(me, keep[:, :, k, :].reshape(shape), recv[:, :, k, :].reshape(shape))
        high, low = split(jnp.concatenate(both, axis=1))
        total = dot(jnp.concatenate([high, low, high], axis=1), stack(s_ref, 0))
        total = total.reshape(2, ny, KB, nz)
        f_out[:, :, k, :] = total
        rows = own_rows(root, base + i, KB)
        lam = root[0, rows, :], root[1, rows, :]
        row = [(total[0, j], total[1, j]) for j in range(ny)]
        p = row[0] if first else cadd(cmul(lam, (before[0, k, :], before[1, k, :])), row[0])
        q = row[ny - 1]
        for j in range(1, ny):
            p = cadd(cmul(lam, p), row[j])
            q = cadd(cmul(lam, q), row[ny - 1 - j])
        if not first:
            q = cadd(cmul(power(lam, ny), q), (before[2, k, :], before[3, k, :]))
            wide = 2 * ny
            left, right = images(lam, 2 * wide, ring, place)
            edge = power(lam, wide + 1)
            p, q = (
                csub(p, cmul(cmul(left, edge), q)),
                csub(q, cmul(cmul(right, edge), p)),
            )
            even = place % 2 == 0
            to = pl.ds(pl.multiple_of(i * KB, KB), KB)
            for c in range(2):
                send[c, to, :] = jnp.where(even, p[c], q[c])
        for c, part in enumerate((*p, *q)):
            pq[c, k, :] = part

    over_blocks(block, nk, (None,) if first else sends)


def over_blocks(block, nk, refs):
    number = nk // KB // len(refs)
    for c, ref in enumerate(refs):

        def step(i, carry, c=c, ref=ref):
            block(ref, c * number, i)
            return carry

        lax.fori_loop(0, number, step, 0)


def csub(a, b):
    return a[0] - b[0], a[1] - b[1]


def images(lam, step, ring, place):
    one, base = (jnp.ones_like(lam[0]), jnp.zeros_like(lam[0])), power(lam, step)
    found = [one, one]
    bit = 1
    while bit < ring:
        for i, number in enumerate((place, ring - 1 - place)):
            taken = (number // bit) % 2 == 1
            more = cmul(found[i], base)
            found[i] = tuple(jnp.where(taken, m, f) for m, f in zip(more, found[i]))
        base, bit = cmul(base, base), 2 * bit
    return found


def fold(chunk, exponent, root, now, recv, out):
    kc = out.shape[1]
    rows = own_rows(root, chunk, kc)
    far = power((root[0, rows, :], root[1, rows, :]), exponent)
    out[0], out[1] = cadd((now[0], now[1]), cmul(far, (recv[0], recv[1])))


def fold_pair(chunk, exponent, root, pq, recv, out):
    kc = out.shape[1]
    rows = own_rows(root, chunk, kc)
    k = pl.ds(chunk * kc, kc)
    far = power((root[0, rows, :], root[1, rows, :]), exponent)
    even = lax.axis_index("px") % 2 == 0
    now = tuple(jnp.where(even, pq[2 + c, k, :], pq[c, k, :]) for c in range(2))
    out[0], out[1] = cadd(now, cmul(far, (recv[0], recv[1])))


def carries(chunk, ny, root, pq, near, one, two, fb):
    kc, ring, place = fb.shape[1], lax.axis_size("px"), lax.axis_index("px")
    rows = own_rows(root, chunk, kc)
    k = pl.ds(chunk * kc, kc)
    lam = root[0, rows, :], root[1, rows, :]
    gam = root[2, rows, :], root[3, rows, :]
    block = power(lam, ny)
    direct = one[0], one[1]
    joined = cadd(cmul(block, (two[0], two[1])), (near[0], near[1]))
    even = place % 2 == 0
    f = tuple(jnp.where(even, a, b) for a, b in zip(direct, joined))
    b = tuple(jnp.where(even, b, a) for a, b in zip(direct, joined))
    p, q = (pq[0, k, :], pq[1, k, :]), (pq[2, k, :], pq[3, k, :])
    left, right = images(lam, 2 * ny, ring, place)
    whole = power(lam, 2 * (ny * ring + 1))
    det = 1.0 - whole[0], -whole[1]
    size = det[0] * det[0] + det[1] * det[1]
    scale = cmul(gam, (det[0] / size, -det[1] / size))
    f, b = (
        csub(f, cmul(cmul(left, lam), cadd(cmul(block, b), q))),
        csub(b, cmul(cmul(right, lam), cadd(cmul(block, f), p))),
    )
    fb[0], fb[1] = cmul(scale, f)
    fb[2], fb[3] = cmul(scale, b)


def local_solve(root, f0, f1, w0, w1):
    _, half, nk, _ = f0.shape
    ny = 2 * half

    def row(refs, j, k):
        ref = refs[j // half]
        return ref[0, j % half, k, :], ref[1, j % half, k, :]

    def block(i, carry):
        k = pl.ds(pl.multiple_of(i * KB, KB), KB)
        rows = own_rows(root, i, KB)
        lam = root[0, rows, :], root[1, rows, :]
        gam = root[2, rows, :], root[3, rows, :]

        def put(j, value):
            ref = (w0, w1)[j // half]
            ref[0, j % half, k, :], ref[1, j % half, k, :] = value

        p = None
        for j in range(ny):
            f = row((f0, f1), j, k)
            p = f if p is None else cadd(cmul(lam, p), f)
            put(j, p)
        q = None
        for j in reversed(range(ny)):
            here = row((w0, w1), j, k)
            if q is None:
                q = row((f0, f1), j, k)
            else:
                q = cmul(lam, q)
                here = cadd(here, q)
                q = cadd(q, row((f0, f1), j, k))
            put(j, cmul(gam, here))
        return carry

    lax.fori_loop(0, nk // KB, block, 0)


def inverse_z(part, s_ref, root, w_ref, *refs):
    *fbs, send, keep, u = refs
    me = lax.axis_index("py")
    _, ny, nk, nz = w_ref.shape
    w = send.shape[3]

    def block(fb, base, i):
        k = pl.ds(pl.multiple_of((base + i) * KB, KB), KB)
        rows = own_rows(root, base + i, KB)
        lam = root[0, rows, :], root[1, rows, :]
        at = pl.ds(pl.multiple_of(i * KB, KB), KB)
        f = fb[0, at, :], fb[1, at, :]
        b = fb[2, at, :], fb[3, at, :]
        past = power(lam, ny)
        if part:
            f = cmul(past, f)
        else:
            b = cmul(past, b)
        for j in range(ny):
            f = cmul(lam, f)
            u[0, j], u[1, j] = cadd((w_ref[0, j, k, :], w_ref[1, j, k, :]), f)
        for j in reversed(range(ny)):
            b = cmul(lam, b)
            u[0, j], u[1, j] = cadd((u[0, j], u[1, j]), b)
        high, low = split(u[...].reshape(2 * ny * KB, nz))
        left = jnp.concatenate([high, low, high], axis=1)
        out = dot(left, stack(s_ref, 0))
        own, away = by_half(me, out[:, :w], out[:, w:])
        send[:, :, k, :] = away.reshape(2, ny, KB, w)
        keep[:, :, k, :] = own.reshape(2, ny, KB, w)

    over_blocks(block, nk, fbs)


def inverse_x(part, s_ref, keep, recv, src, speed, out, sums):
    me = lax.axis_index("py")
    _, nx, _, w = out.shape
    left = stack(s_ref, 1)
    for c in range(2):
        cols = []
        for y in range(YB):
            high, low = split(jnp.concatenate(by_half(me, keep[c, y], recv[c, y]), axis=0))
            cols.append(jnp.concatenate([high, low, high], axis=0))
        got = dot(left, jnp.concatenate(cols, axis=1))
        flat = out.at[c].reshape(nx * YB, w)
        for y in range(YB):
            flat[pl.ds(y, nx, stride=YB), :] = got[:, y * w : (y + 1) * w]
    here = pl.ds(part * YB, YB)
    damped = damping * wave_square

    def step(i, acc):
        s0, s1 = src[0, i, here, :], src[1, i, here, :]
        p0, p1 = out[0, i], out[1, i]
        c = speed[i, here, :]
        factor = wave_square - wave_square / (c * c)
        a0 = s0 + factor * p0 + damped * p1
        a1 = s1 + factor * p1 - damped * p0
        new = (
            s0 * s0 + s1 * s1,
            s0 * a0 + s1 * a1,
            s0 * a1 - s1 * a0,
            a0 * a0 + a1 * a1,
        )
        return tuple(x + y for x, y in zip(acc, new))

    zero = jnp.zeros((YB, w), f32)
    acc = lax.fori_loop(0, nx, step, (zero,) * 4, unroll=8)
    for i, a in enumerate(acc):
        sums[i : i + 1, :] = jnp.sum(a, axis=0, keepdims=True)


def finish(total, ps0, ps1, out_hbm, scaled, sems):
    sums = jnp.sum(jnp.sum(total[...], axis=0), axis=1, keepdims=True)
    square, re, im, size = (sums[i : i + 1] for i in range(4))
    beta2 = square + epsilon
    re, im, size = re / beta2, im / beta2, size / beta2
    den = size - (re * re + im * im) * (epsilon / beta2) + epsilon
    a, b = re / den, -im / den
    _, nx, _, w = ps0.shape
    a = jnp.broadcast_to(a, (YB, w))
    b = jnp.broadcast_to(b, (YB, w))
    copies = []
    for part, ps in enumerate((ps0, ps1)):
        for x in range(0, nx, XC):

            def step(i, carry, part=part, ps=ps):
                p0, p1 = ps[0, i], ps[1, i]
                scaled[part, 0, i] = a * p0 - b * p1
                scaled[part, 1, i] = a * p1 + b * p0
                return carry

            lax.fori_loop(x, x + XC, step, 0, unroll=8)
            copy = pltpu.make_async_copy(
                scaled.at[part, :, pl.ds(x, XC)],
                out_hbm.at[:, pl.ds(x, XC), pl.ds(part * YB, YB), :],
                sems.at[len(copies)],
            )
            copy.start()
            copies.append(copy)
    for copy in copies:
        copy.wait()


def params(mib, *dims):
    return pltpu.CompilerParams(dimension_semantics=dims or None, vmem_limit_bytes=mib * 2**20)


def whole(a):
    return pl.BlockSpec(a.shape, lambda *_: (0,) * a.ndim)


VM = pl.BlockSpec(memory_space=pltpu.VMEM)
ANY = pl.BlockSpec(memory_space=pl.ANY)


def cost(flops, moved):
    return pl.CostEstimate(flops=flops, bytes_accessed=moved, transcendentals=0)


def on_device(source, speed):
    _, nx, ny, w = source.shape
    cores, ring = lax.axis_size("py"), lax.axis_size("px")
    nz, nk = w * cores, nx // cores
    other = [(i, cores - 1 - i) for i in range(cores)]
    sds = lambda *shape: jax.ShapeDtypeStruct(shape, f32)

    table_x = jnp.asarray(np.stack(halves_of(sine_table(nx))))
    table_z = table_x if nz == nx else jnp.asarray(np.stack(halves_of(sine_table(nz))))
    root = jnp.asarray(root_tables(nx, nz))
    piece = sds(2, YB, nk, w)
    modes = sds(2, YB, nk, nz)
    flops = 2 * 2 * nx * YB * w * nx * 3
    est = cost(flops, 4 * 2**20)

    moved = []
    for h in range(2):
        send, keep = pl.pallas_call(
            functools.partial(forward_x, h),
            in_specs=[VM] * 2,
            out_specs=[VM] * 2,
            out_shape=[piece, piece],
            compiler_params=params(12),
            cost_estimate=est,
            name="forward_x",
        )(table_x, source)
        moved.append((keep, lax.ppermute(send, "py", other)))
    f, before = [], ()
    kc = nk // CHUNKS
    plane = sds(2, kc, nz)
    for h in range(2):
        got, pq, *sends = pl.pallas_call(
            functools.partial(forward_z, h == 0),
            in_specs=[VM] * (4 + len(before)),
            out_specs=[VM] * (2 + h * CHUNKS),
            out_shape=[modes, sds(4, nk, nz)] + [plane] * (h * CHUNKS),
            compiler_params=params(12),
            cost_estimate=est,
            name="forward_z",
        )(table_z, root, *moved[h], *before)
        f.append(got)
        before = (pq,)

    def small(body, n_in, out, name):
        return pl.pallas_call(
            body,
            in_specs=[VM] * n_in,
            out_specs=VM,
            out_shape=out,
            compiler_params=params(4),
            cost_estimate=cost(2 * 10**6, 2**19),
            name=name,
        )

    def mirrored(pairs):
        return pairs + [(ring - 1 - a, ring - 1 - b) for a, b in pairs]

    pair = mirrored([(i, i + 1) for i in range(0, ring, 2)])
    quad = mirrored([(i, i + 2) for i in range(1, ring, 4)])
    hops = [mirrored([(i, i + 4)]) for i in range(3, ring - 5, 4)]
    down = mirrored([(i, i + 2) for i in range(3, ring - 2, 4)])
    sums = [lax.ppermute(s, "px", pair) for s in sends]
    near = sums
    now = [small(functools.partial(fold_pair, c, ny), 3, plane, "fold")(root, pq, r) for c, r in enumerate(near)]
    for route, blocks in [(quad, 2)] + [(hop, 4) for hop in hops] + [(down, 2)]:
        sums = [lax.ppermute(s, "px", route) for s in now]
        now = [
            small(functools.partial(fold, c, blocks * ny), 3, plane, "fold")(root, s, r)
            for c, (s, r) in enumerate(zip(now, sums))
        ]
    two = [lax.ppermute(s, "px", mirrored([(i, i + 2) for i in range(1, ring - 2, 2)])) for s in now]
    one = [lax.ppermute(s, "px", mirrored([(i, i + 1) for i in range(1, ring - 2, 2)])) for s in now]
    fb = [
        small(functools.partial(carries, c, ny), 5, sds(4, kc, nz), "carries")(root, pq, near[c], one[c], two[c])
        for c in range(CHUNKS)
    ]
    local = pl.pallas_call(
        local_solve,
        in_specs=[VM] * 3,
        out_specs=[VM, VM],
        out_shape=[modes, modes],
        compiler_params=params(8),
        cost_estimate=cost(2 * flops, 8 * 2**20),
        name="local_solve",
    )(root, *f)
    moved = []
    for h in range(2):
        send, keep = pl.pallas_call(
            functools.partial(inverse_z, h),
            in_specs=[VM] * (3 + CHUNKS),
            out_specs=[VM, VM],
            out_shape=[piece, piece],
            scratch_shapes=[pltpu.VMEM((2, YB, KB, nz), f32)],
            compiler_params=params(12),
            cost_estimate=est,
            name="inverse_z",
        )(table_z, root, local[h], *fb)
        moved.append((keep, lax.ppermute(send, "py", other)))
    solved, sums = [], []
    for h in range(2):
        got, part = pl.pallas_call(
            functools.partial(inverse_x, h),
            in_specs=[VM] * 5,
            out_specs=[VM, VM],
            out_shape=[sds(2, nx, YB, w), sds(4, w)],
            compiler_params=params(16),
            cost_estimate=est,
            name="inverse_x",
        )(table_x, *moved[h], source, speed)
        solved.append(got)
        sums.append(part)
    sums = sums[0] + sums[1]
    sums = sums + lax.ppermute(sums, "py", other)
    every = lax.all_to_all(jnp.broadcast_to(sums[None], (ring, 4, w)), "px", 0, 0, tiled=True)
    return pl.pallas_call(
        finish,
        in_specs=[VM] * 3,
        out_specs=ANY,
        out_shape=sds(*source.shape),
        scratch_shapes=[pltpu.VMEM((2, 2, nx, YB, w), f32), pltpu.SemaphoreType.DMA((2 * nx // XC,))],
        compiler_params=params(16),
        cost_estimate=cost(10**7, 8 * 2**20),
        name="finish",
    )(every, *solved)


def solution(mesh):
    return jax.shard_map(
        on_device,
        mesh=mesh,
        in_specs=(P(None, "samples", "px", "py"), P("samples", "px", "py")),
        out_specs=P(None, "samples", "px", "py"),
        check_vma=False,
    )
```

```python
import functools
import numpy as np
import jax
import jax.numpy as jnp
from jax import lax
from jax.experimental import pallas as pl
from jax.experimental.pallas import tpu as pltpu
from jax.sharding import PartitionSpec as P

wave_square = 0.25
damping = 0.5
epsilon = 1e-06
f32 = jnp.float32
bf16 = jnp.bfloat16
YB = 8
KB = 32
XC = 32
CHUNKS = 2


def sine_table(length):
    k = np.arange(1, length + 1, dtype=np.float64)
    phases = np.mod(np.outer(k, k), 2 * (length + 1)) * (np.pi / (length + 1))
    return np.sqrt(2.0 / (length + 1)) * np.sin(phases)


def halves_of(table):
    table = table.astype(np.float32)
    high = table.astype(bf16)
    low = (table - high.astype(np.float32)).astype(bf16)
    return high, low


def eigen_line(length):
    k = np.arange(1, length + 1, dtype=np.float64)
    return 4.0 * np.sin(np.pi * k / (2.0 * (length + 1))) ** 2


def root_tables(nx, nz):
    near = eigen_line(nx)[:, None] + eigen_line(nz)[None, :] - wave_square + 1j * damping * wave_square
    spread = np.sqrt(near) * np.sqrt(near + 4.0)
    lam = 2.0 / (near + 2.0 + spread)
    gam = 1.0 / spread
    return np.stack([lam.real, lam.imag, gam.real, gam.imag]).astype(np.float32)


def cmul(a, b):
    return a[0] * b[0] - a[1] * b[1], a[0] * b[1] + a[1] * b[0]


def cadd(a, b):
    return a[0] + b[0], a[1] + b[1]


def split(v):
    high = v.astype(bf16)
    return high, (v - high.astype(f32)).astype(bf16)


def dot(a, b):
    return lax.dot_general(a, b, (((1,), (0,)), ((), ())), preferred_element_type=f32)


def stack(s_ref, axis):
    return jnp.concatenate([s_ref[0], s_ref[0], s_ref[1]], axis=axis)


def by_half(me, keep, recv):
    first = me == 0
    return jnp.where(first, keep, recv), jnp.where(first, recv, keep)


def forward_x(part, s_ref, src, send, keep):
    me = lax.axis_index("py")
    _, nx, ny, w = src.shape
    nk = nx // 2
    for c in range(2):
        flat = src.at[c].reshape(nx * ny, w)
        cols = []
        for y in range(YB):
            high, low = split(flat[pl.ds(part * YB + y, nx, stride=ny), :])
            cols.append(jnp.concatenate([high, low, high], axis=0))
        right = jnp.concatenate(cols, axis=1)
        for half, out in ((1 - me, send), (me, keep)):
            rows = pl.ds(pl.multiple_of(half * nk, nk), nk)
            high, low = s_ref[0, rows, :], s_ref[1, rows, :]
            got = dot(jnp.concatenate([high, high, low], axis=1), right)
            for y in range(YB):
                out[c, y] = got[:, y * w : (y + 1) * w]


def own_rows(root, block, kb):
    nk = root.shape[1] // 2
    return pl.ds(pl.multiple_of(lax.axis_index("py") * nk + block * kb, kb), kb)


def power(base, exponent):
    result = None
    while exponent:
        if exponent & 1:
            result = base if result is None else cmul(result, base)
        exponent >>= 1
        if exponent:
            base = cmul(base, base)
    return result


def forward_z(chunk, first, s_ref, root, keep, recv, *refs):
    if first:
        f_out, pq = refs
    else:
        before, f_out, pq, send = refs
    me = lax.axis_index("py")
    ring, place = lax.axis_size("px"), lax.axis_index("px")
    _, ny, _, w = keep.shape
    _, _, kc, nz = f_out.shape

    def block(i, carry):
        k = pl.ds(pl.multiple_of(i * KB, KB), KB)
        here = pl.ds(pl.multiple_of(chunk * kc + i * KB, KB), KB)
        shape = 2 * ny * KB, w
        both = by_half(me, keep[:, :, here, :].reshape(shape), recv[:, :, here, :].reshape(shape))
        high, low = split(jnp.concatenate(both, axis=1))
        total = dot(jnp.concatenate([high, low, high], axis=1), stack(s_ref, 0))
        total = total.reshape(2, ny, KB, nz)
        f_out[:, :, k, :] = total
        rows = own_rows(root, chunk * (kc // KB) + i, KB)
        lam = root[0, rows, :], root[1, rows, :]
        row = [(total[0, j], total[1, j]) for j in range(ny)]
        p = row[0] if first else cadd(cmul(lam, (before[0, k, :], before[1, k, :])), row[0])
        q = row[ny - 1]
        for j in range(1, ny):
            p = cadd(cmul(lam, p), row[j])
            q = cadd(cmul(lam, q), row[ny - 1 - j])
        if not first:
            q = cadd(cmul(power(lam, ny), q), (before[2, k, :], before[3, k, :]))
            wide = 2 * ny
            left, right = images(lam, 2 * wide, ring, place)
            edge = power(lam, wide + 1)
            p, q = (
                csub(p, cmul(cmul(left, edge), q)),
                csub(q, cmul(cmul(right, edge), p)),
            )
            even = place % 2 == 0
            for c in range(2):
                send[c, k, :] = jnp.where(even, p[c], q[c])
        for c, part in enumerate((*p, *q)):
            pq[c, k, :] = part
        return carry

    lax.fori_loop(0, kc // KB, block, 0)


def csub(a, b):
    return a[0] - b[0], a[1] - b[1]


def images(lam, step, ring, place):
    one, base = (jnp.ones_like(lam[0]), jnp.zeros_like(lam[0])), power(lam, step)
    found = [one, one]
    bit = 1
    while bit < ring:
        for i, number in enumerate((place, ring - 1 - place)):
            taken = (number // bit) % 2 == 1
            more = cmul(found[i], base)
            found[i] = tuple(jnp.where(taken, m, f) for m, f in zip(more, found[i]))
        base, bit = cmul(base, base), 2 * bit
    return found


def fold(chunk, exponents, root, now, *refs):
    *recv, out = refs
    kc = out.shape[1]
    rows = own_rows(root, chunk, kc)
    total = now[0], now[1]
    for exponent, r in zip(exponents, recv):
        far = power((root[0, rows, :], root[1, rows, :]), exponent)
        total = cadd(total, cmul(far, (r[0], r[1])))
    out[0], out[1] = total


def fold_pair(chunk, exponent, root, pq, recv, out):
    kc = out.shape[1]
    rows = own_rows(root, chunk, kc)
    far = power((root[0, rows, :], root[1, rows, :]), exponent)
    even = lax.axis_index("px") % 2 == 0
    now = tuple(jnp.where(even, pq[2 + c], pq[c]) for c in range(2))
    out[0], out[1] = cadd(now, cmul(far, (recv[0], recv[1])))


def carries(chunk, ny, root, pq, near, one, two, fb):
    kc, ring, place = fb.shape[1], lax.axis_size("px"), lax.axis_index("px")
    rows = own_rows(root, chunk, kc)
    lam = root[0, rows, :], root[1, rows, :]
    gam = root[2, rows, :], root[3, rows, :]
    block = power(lam, ny)
    direct = one[0], one[1]
    joined = cadd(cmul(block, (two[0], two[1])), (near[0], near[1]))
    even = place % 2 == 0
    f = tuple(jnp.where(even, a, b) for a, b in zip(direct, joined))
    b = tuple(jnp.where(even, b, a) for a, b in zip(direct, joined))
    p, q = (pq[0], pq[1]), (pq[2], pq[3])
    left, right = images(lam, 2 * ny, ring, place)
    whole = power(lam, 2 * (ny * ring + 1))
    det = 1.0 - whole[0], -whole[1]
    size = det[0] * det[0] + det[1] * det[1]
    scale = cmul(gam, (det[0] / size, -det[1] / size))
    f, b = (
        csub(f, cmul(cmul(left, lam), cadd(cmul(block, b), q))),
        csub(b, cmul(cmul(right, lam), cadd(cmul(block, f), p))),
    )
    fb[0], fb[1] = cmul(scale, f)
    fb[2], fb[3] = cmul(scale, b)


def local_solve(chunk, root, f0, f1, w0, w1):
    _, half, kc, _ = f0.shape
    ny = 2 * half

    def row(refs, j, k):
        ref = refs[j // half]
        return ref[0, j % half, k, :], ref[1, j % half, k, :]

    def block(i, carry):
        k = pl.ds(pl.multiple_of(i * KB, KB), KB)
        rows = own_rows(root, chunk * (kc // KB) + i, KB)
        lam = root[0, rows, :], root[1, rows, :]
        gam = root[2, rows, :], root[3, rows, :]

        def put(j, value):
            ref = (w0, w1)[j // half]
            ref[0, j % half, k, :], ref[1, j % half, k, :] = value

        p = None
        for j in range(ny):
            f = row((f0, f1), j, k)
            p = f if p is None else cadd(cmul(lam, p), f)
            put(j, p)
        q = None
        for j in reversed(range(ny)):
            here = row((w0, w1), j, k)
            if q is None:
                q = row((f0, f1), j, k)
            else:
                q = cmul(lam, q)
                here = cadd(here, q)
                q = cadd(q, row((f0, f1), j, k))
            put(j, cmul(gam, here))
        return carry

    lax.fori_loop(0, kc // KB, block, 0)


def inverse_z(chunk, part, s_ref, root, w_ref, fb, send, keep, u):
    me = lax.axis_index("py")
    _, ny, kc, nz = w_ref.shape
    w = send.shape[3]

    def block(i, carry):
        k = pl.ds(pl.multiple_of(i * KB, KB), KB)
        rows = own_rows(root, chunk * (kc // KB) + i, KB)
        lam = root[0, rows, :], root[1, rows, :]
        f = fb[0, k, :], fb[1, k, :]
        b = fb[2, k, :], fb[3, k, :]
        past = power(lam, ny)
        if part:
            f = cmul(past, f)
        else:
            b = cmul(past, b)
        for j in range(ny):
            f = cmul(lam, f)
            u[0, j], u[1, j] = cadd((w_ref[0, j, k, :], w_ref[1, j, k, :]), f)
        for j in reversed(range(ny)):
            b = cmul(lam, b)
            u[0, j], u[1, j] = cadd((u[0, j], u[1, j]), b)
        high, low = split(u[...].reshape(2 * ny * KB, nz))
        left = jnp.concatenate([high, low, high], axis=1)
        out = dot(left, stack(s_ref, 0))
        own, away = by_half(me, out[:, :w], out[:, w:])
        send[:, :, k, :] = away.reshape(2, ny, KB, w)
        keep[:, :, k, :] = own.reshape(2, ny, KB, w)
        return carry

    lax.fori_loop(0, kc // KB, block, 0)


def inverse_x(part, s_ref, *refs):
    *moved, src, speed, out, sums = refs
    number = len(moved) // 2
    me = lax.axis_index("py")
    _, nx, _, w = out.shape
    left = stack(s_ref, 1)
    for c in range(2):
        cols = []
        for y in range(YB):
            keep, recv = (jnp.concatenate([r[c, y] for r in rs], axis=0) for rs in (moved[:number], moved[number:]))
            high, low = split(jnp.concatenate(by_half(me, keep, recv), axis=0))
            cols.append(jnp.concatenate([high, low, high], axis=0))
        got = dot(left, jnp.concatenate(cols, axis=1))
        flat = out.at[c].reshape(nx * YB, w)
        for y in range(YB):
            flat[pl.ds(y, nx, stride=YB), :] = got[:, y * w : (y + 1) * w]
    here = pl.ds(part * YB, YB)
    damped = damping * wave_square

    def step(i, acc):
        s0, s1 = src[0, i, here, :], src[1, i, here, :]
        p0, p1 = out[0, i], out[1, i]
        c = speed[i, here, :]
        factor = wave_square - wave_square / (c * c)
        a0 = s0 + factor * p0 + damped * p1
        a1 = s1 + factor * p1 - damped * p0
        new = (
            s0 * s0 + s1 * s1,
            s0 * a0 + s1 * a1,
            s0 * a1 - s1 * a0,
            a0 * a0 + a1 * a1,
        )
        return tuple(x + y for x, y in zip(acc, new))

    zero = jnp.zeros((YB, w), f32)
    acc = lax.fori_loop(0, nx, step, (zero,) * 4, unroll=8)
    for i, a in enumerate(acc):
        sums[i : i + 1, :] = jnp.sum(a, axis=0, keepdims=True)


def finish(total, ps0, ps1, out_hbm, scaled, sems):
    sums = jnp.sum(jnp.sum(total[...], axis=0), axis=1, keepdims=True)
    square, re, im, size = (sums[i : i + 1] for i in range(4))
    beta2 = square + epsilon
    re, im, size = re / beta2, im / beta2, size / beta2
    den = size - (re * re + im * im) * (epsilon / beta2) + epsilon
    a, b = re / den, -im / den
    _, nx, _, w = ps0.shape
    a = jnp.broadcast_to(a, (YB, w))
    b = jnp.broadcast_to(b, (YB, w))
    copies = []
    for part, ps in enumerate((ps0, ps1)):
        for x in range(0, nx, XC):

            def step(i, carry, part=part, ps=ps):
                p0, p1 = ps[0, i], ps[1, i]
                scaled[part, 0, i] = a * p0 - b * p1
                scaled[part, 1, i] = a * p1 + b * p0
                return carry

            lax.fori_loop(x, x + XC, step, 0, unroll=8)
            copy = pltpu.make_async_copy(
                scaled.at[part, :, pl.ds(x, XC)],
                out_hbm.at[:, pl.ds(x, XC), pl.ds(part * YB, YB), :],
                sems.at[len(copies)],
            )
            copy.start()
            copies.append(copy)
    for copy in copies:
        copy.wait()


def params(mib, *dims):
    return pltpu.CompilerParams(dimension_semantics=dims or None, vmem_limit_bytes=mib * 2**20)


def whole(a):
    return pl.BlockSpec(a.shape, lambda *_: (0,) * a.ndim)


VM = pl.BlockSpec(memory_space=pltpu.VMEM)
ANY = pl.BlockSpec(memory_space=pl.ANY)


def cost(flops, moved):
    return pl.CostEstimate(flops=flops, bytes_accessed=moved, transcendentals=0)


def on_device(source, speed):
    _, nx, ny, w = source.shape
    cores, ring = lax.axis_size("py"), lax.axis_size("px")
    nz, nk = w * cores, nx // cores
    other = [(i, cores - 1 - i) for i in range(cores)]
    sds = lambda *shape: jax.ShapeDtypeStruct(shape, f32)

    table_x = jnp.asarray(np.stack(halves_of(sine_table(nx))))
    table_z = table_x if nz == nx else jnp.asarray(np.stack(halves_of(sine_table(nz))))
    root = jnp.asarray(root_tables(nx, nz))
    piece = sds(2, YB, nk, w)
    flops = 2 * 2 * nx * YB * w * nx * 3
    est = cost(flops, 4 * 2**20)

    moved = []
    for h in range(2):
        send, keep = pl.pallas_call(
            functools.partial(forward_x, h),
            in_specs=[VM] * 2,
            out_specs=[VM] * 2,
            out_shape=[piece, piece],
            compiler_params=params(12),
            cost_estimate=est,
            name="forward_x",
        )(table_x, source)
        moved.append((keep, lax.ppermute(send, "py", other)))
    kc = nk // CHUNKS
    plane, block = sds(2, kc, nz), sds(2, YB, kc, nz)
    f, pq, sends = {}, [()] * CHUNKS, []
    for h in range(2):
        for c in range(CHUNKS):
            before = () if h == 0 else (pq[c],)
            f[h, c], pq[c], *send = pl.pallas_call(
                functools.partial(forward_z, c, h == 0),
                in_specs=[VM] * (4 + h),
                out_specs=[VM] * (2 + h),
                out_shape=[block, sds(4, kc, nz)] + [plane] * h,
                compiler_params=params(12),
                cost_estimate=est,
                name="forward_z",
            )(table_z, root, *moved[h], *before)
            sends += send

    def small(body, n_in, out, name):
        return pl.pallas_call(
            body,
            in_specs=[VM] * n_in,
            out_specs=VM,
            out_shape=out,
            compiler_params=params(4),
            cost_estimate=cost(2 * 10**6, 2**19),
            name=name,
        )

    def mirrored(pairs):
        return pairs + [(ring - 1 - a, ring - 1 - b) for a, b in pairs]

    pair = mirrored([(i, i + 1) for i in range(0, ring, 2)])
    quad = mirrored([(i, i + 2) for i in range(1, ring, 4)])
    steps = range(1, ring // 4 - 1)
    hops = [mirrored([(4 * m - 1, 4 * m + 3)]) for m in steps]
    down = mirrored([(i, i + 2) for i in range(3, ring - 2, 4)])
    local = [
        pl.pallas_call(
            functools.partial(local_solve, c),
            in_specs=[VM] * 3,
            out_specs=[VM, VM],
            out_shape=[block, block],
            compiler_params=params(8),
            cost_estimate=cost(flops // 8, 8 * 2**20),
            name="local_solve",
        )(root, f[0, c], f[1, c])
        for c in range(CHUNKS)
    ]
    near = [lax.ppermute(s, "px", pair) for s in sends]
    now = [small(functools.partial(fold_pair, c, ny), 3, plane, "fold")(root, pq[c], r) for c, r in enumerate(near)]
    for level, (route, blocks) in enumerate([(quad, 2)] + [(hop, 4) for hop in hops] + [(down, 2)]):
        for c, s in enumerate(now):
            recv = lax.ppermute(s, "px", route)
            if level == 1:
                recv, local[c] = lax.optimization_barrier((recv, local[c]))
            now[c] = small(functools.partial(fold, c, [ny * blocks]), 3, plane, "fold")(root, s, recv)
    one = [lax.ppermute(s, "px", mirrored([(i, i + 1) for i in range(1, ring - 2, 2)])) for s in now]
    two = [lax.ppermute(s, "px", pair) for s in one]
    fb = [
        small(functools.partial(carries, c, ny), 5, sds(4, kc, nz), "carries")(root, pq[c], near[c], one[c], two[c])
        for c in range(CHUNKS)
    ]
    kept, sent = {}, {}
    half = sds(2, YB, kc, w)
    for h in range(2):
        for c in range(CHUNKS):
            send, kept[h, c] = pl.pallas_call(
                functools.partial(inverse_z, c, h),
                in_specs=[VM] * 4,
                out_specs=[VM, VM],
                out_shape=[half, half],
                scratch_shapes=[pltpu.VMEM((2, YB, KB, nz), f32)],
                compiler_params=params(12),
                cost_estimate=est,
                name="inverse_z",
            )(table_z, root, local[c][h], fb[c])
            sent[h, c] = lax.ppermute(send, "py", other)
    solved, sums = [], []
    for h in range(2):
        got, part = pl.pallas_call(
            functools.partial(inverse_x, h),
            in_specs=[VM] * (3 + 2 * CHUNKS),
            out_specs=[VM, VM],
            out_shape=[sds(2, nx, YB, w), sds(4, w)],
            compiler_params=params(16),
            cost_estimate=est,
            name="inverse_x",
        )(table_x, *(kept[h, c] for c in range(CHUNKS)), *(sent[h, c] for c in range(CHUNKS)), source, speed)
        solved.append(got)
        sums.append(part)
    sums = sums[0] + sums[1]
    sums = sums + lax.ppermute(sums, "py", other)
    every = lax.all_to_all(jnp.broadcast_to(sums[None], (ring, 4, w)), "px", 0, 0, tiled=True)
    return pl.pallas_call(
        finish,
        in_specs=[VM] * 3,
        out_specs=ANY,
        out_shape=sds(*source.shape),
        scratch_shapes=[pltpu.VMEM((2, 2, nx, YB, w), f32), pltpu.SemaphoreType.DMA((2 * nx // XC,))],
        compiler_params=params(16),
        cost_estimate=cost(10**7, 8 * 2**20),
        name="finish",
    )(every, *solved)


def solution(mesh):
    return jax.shard_map(
        on_device,
        mesh=mesh,
        in_specs=(P(None, "samples", "px", "py"), P("samples", "px", "py")),
        out_specs=P(None, "samples", "px", "py"),
        check_vma=False,
    )
```

```python
import functools
import numpy as np
import jax
import jax.numpy as jnp
from jax import lax
from jax.experimental import pallas as pl
from jax.experimental.pallas import tpu as pltpu
from jax.sharding import PartitionSpec as P

wave_square = 0.25
damping = 0.5
epsilon = 1e-06
f32 = jnp.float32
bf16 = jnp.bfloat16
YB = 8
KB = 32
XC = 32
CHUNKS = 2


def sine_table(length):
    k = np.arange(1, length + 1, dtype=np.float64)
    phases = np.mod(np.outer(k, k), 2 * (length + 1)) * (np.pi / (length + 1))
    return np.sqrt(2.0 / (length + 1)) * np.sin(phases)


def halves_of(table):
    table = table.astype(np.float32)
    high = table.astype(bf16)
    low = (table - high.astype(np.float32)).astype(bf16)
    return high, low


def eigen_line(length):
    k = np.arange(1, length + 1, dtype=np.float64)
    return 4.0 * np.sin(np.pi * k / (2.0 * (length + 1))) ** 2


def root_tables(nx, nz):
    near = eigen_line(nx)[:, None] + eigen_line(nz)[None, :] - wave_square + 1j * damping * wave_square
    spread = np.sqrt(near) * np.sqrt(near + 4.0)
    lam = 2.0 / (near + 2.0 + spread)
    gam = 1.0 / spread
    return np.stack([lam.real, lam.imag, gam.real, gam.imag]).astype(np.float32)


def cmul(a, b):
    return a[0] * b[0] - a[1] * b[1], a[0] * b[1] + a[1] * b[0]


def cadd(a, b):
    return a[0] + b[0], a[1] + b[1]


def split(v):
    high = v.astype(bf16)
    return high, (v - high.astype(f32)).astype(bf16)


def dot(a, b):
    return lax.dot_general(a, b, (((1,), (0,)), ((), ())), preferred_element_type=f32)


def stack(s_ref, axis):
    return jnp.concatenate([s_ref[0], s_ref[0], s_ref[1]], axis=axis)


def by_half(me, keep, recv):
    first = me == 0
    return jnp.where(first, keep, recv), jnp.where(first, recv, keep)


def forward_x(chunk, s_ref, values, send, keep, *parts):
    me = lax.axis_index("py")
    _, ny, kc, w = send.shape
    nx = s_ref.shape[1]
    for h in range(ny // YB):
        for c in range(2):
            if parts:
                flat = values.at[c].reshape(nx * ny, w)
                cols = []
                for y in range(YB):
                    cols.append(jnp.concatenate(split(flat[pl.ds(h * YB + y, nx, stride=ny), :]), axis=0))
                both = jnp.concatenate(cols, axis=1)
                parts[0][c, h] = both
            else:
                both = values[c, h]
            right = jnp.concatenate([both, both[:nx]], axis=0)
            left = []
            for half in (1 - me, me):
                rows = pl.ds(pl.multiple_of(half * (nx // 2) + chunk * kc, kc), kc)
                high, low = s_ref[0, rows, :], s_ref[1, rows, :]
                left.append(jnp.concatenate([high, high, low], axis=1))
            got = dot(jnp.concatenate(left, axis=0), right)
            for y in range(YB):
                send[c, h * YB + y] = got[:kc, y * w : (y + 1) * w]
                keep[c, h * YB + y] = got[kc:, y * w : (y + 1) * w]


def own_rows(root, block, kb):
    nk = root.shape[1] // 2
    return pl.ds(pl.multiple_of(lax.axis_index("py") * nk + block * kb, kb), kb)


def power(base, exponent):
    result = None
    while exponent:
        if exponent & 1:
            result = base if result is None else cmul(result, base)
        exponent >>= 1
        if exponent:
            base = cmul(base, base)
    return result


def forward_z(chunk, s_ref, root, keep, recv, *refs):
    *_, f0, f1, pq, send, done = refs
    done[...] = jnp.zeros_like(done)
    me = lax.axis_index("py")
    ring, place = lax.axis_size("px"), lax.axis_index("px")
    _, ny, kc, w = keep.shape
    nz = f0.shape[3]

    def block(i, carry):
        k = pl.ds(pl.multiple_of(i * KB, KB), KB)
        rows = own_rows(root, chunk * (kc // KB) + i, KB)
        lam = root[0, rows, :], root[1, rows, :]
        p, q = None, None
        for h, f in enumerate((f0, f1)):
            here = slice(h * YB, (h + 1) * YB)
            shape = 2 * YB * KB, w
            both = by_half(me, keep[:, here, k, :].reshape(shape), recv[:, here, k, :].reshape(shape))
            high, low = split(jnp.concatenate(both, axis=1))
            total = dot(jnp.concatenate([high, low, high], axis=1), stack(s_ref, 0))
            total = total.reshape(2, YB, KB, nz)
            f[:, :, k, :] = total
            row = [(total[0, j], total[1, j]) for j in range(YB)]
            p = row[0] if p is None else cadd(cmul(lam, p), row[0])
            part = row[YB - 1]
            for j in range(1, YB):
                p = cadd(cmul(lam, p), row[j])
                part = cadd(cmul(lam, part), row[YB - 1 - j])
            q = part if q is None else cadd(cmul(power(lam, h * YB), part), q)
        left, right = images(lam, 2 * ny, ring, place)
        edge = power(lam, ny + 1)
        p, q = (
            csub(p, cmul(cmul(left, edge), q)),
            csub(q, cmul(cmul(right, edge), p)),
        )
        even = place % 2 == 0
        for c in range(2):
            send[c, k, :] = jnp.where(even, p[c], q[c])
        for c, part in enumerate((*p, *q)):
            pq[c, k, :] = part
        return carry

    lax.fori_loop(0, kc // KB, block, 0)


def csub(a, b):
    return a[0] - b[0], a[1] - b[1]


def images(lam, step, ring, place):
    one, base = (jnp.ones_like(lam[0]), jnp.zeros_like(lam[0])), power(lam, step)
    found = [one, one]
    bit = 1
    while bit < ring:
        for i, number in enumerate((place, ring - 1 - place)):
            taken = (number // bit) % 2 == 1
            more = cmul(found[i], base)
            found[i] = tuple(jnp.where(taken, m, f) for m, f in zip(more, found[i]))
        base, bit = cmul(base, base), 2 * bit
    return found


def fold(chunk, exponents, root, now, *refs):
    *recv, out = refs
    kc = out.shape[1]
    rows = own_rows(root, chunk, kc)
    total = now[0], now[1]
    for exponent, r in zip(exponents, recv):
        far = power((root[0, rows, :], root[1, rows, :]), exponent)
        total = cadd(total, cmul(far, (r[0], r[1])))
    out[0], out[1] = total


def fold_pair(chunk, exponent, root, pq, recv, *refs):
    *_, out, done = refs
    done[...] = jnp.zeros_like(done)
    kc = out.shape[1]
    rows = own_rows(root, chunk, kc)
    far = power((root[0, rows, :], root[1, rows, :]), exponent)
    even = lax.axis_index("px") % 2 == 0
    now = tuple(jnp.where(even, pq[2 + c], pq[c]) for c in range(2))
    out[0], out[1] = cadd(now, cmul(far, (recv[0], recv[1])))


def carries(chunk, ny, root, pq, near, one, two, fb):
    kc, ring, place = fb.shape[1], lax.axis_size("px"), lax.axis_index("px")
    rows = own_rows(root, chunk, kc)
    lam = root[0, rows, :], root[1, rows, :]
    gam = root[2, rows, :], root[3, rows, :]
    block = power(lam, ny)
    direct = one[0], one[1]
    joined = cadd(cmul(block, (two[0], two[1])), (near[0], near[1]))
    even = place % 2 == 0
    f = tuple(jnp.where(even, a, b) for a, b in zip(direct, joined))
    b = tuple(jnp.where(even, b, a) for a, b in zip(direct, joined))
    p, q = (pq[0], pq[1]), (pq[2], pq[3])
    left, right = images(lam, 2 * ny, ring, place)
    whole = power(lam, 2 * (ny * ring + 1))
    det = 1.0 - whole[0], -whole[1]
    size = det[0] * det[0] + det[1] * det[1]
    scale = cmul(gam, (det[0] / size, -det[1] / size))
    f, b = (
        csub(f, cmul(cmul(left, lam), cadd(cmul(block, b), q))),
        csub(b, cmul(cmul(right, lam), cadd(cmul(block, f), p))),
    )
    fb[0], fb[1] = cmul(scale, f)
    fb[2], fb[3] = cmul(scale, b)


def local_solve(chunk, root, f0, f1, w0, w1):
    _, half, kc, _ = f0.shape
    ny = 2 * half

    def row(refs, j, k):
        ref = refs[j // half]
        return ref[0, j % half, k, :], ref[1, j % half, k, :]

    def block(i, carry):
        k = pl.ds(pl.multiple_of(i * KB, KB), KB)
        rows = own_rows(root, chunk * (kc // KB) + i, KB)
        lam = root[0, rows, :], root[1, rows, :]
        gam = root[2, rows, :], root[3, rows, :]

        def put(j, value):
            ref = (w0, w1)[j // half]
            ref[0, j % half, k, :], ref[1, j % half, k, :] = value

        p = None
        for j in range(ny):
            f = row((f0, f1), j, k)
            p = f if p is None else cadd(cmul(lam, p), f)
            put(j, p)
        q = None
        for j in reversed(range(ny)):
            here = row((w0, w1), j, k)
            if q is None:
                q = row((f0, f1), j, k)
            else:
                q = cmul(lam, q)
                here = cadd(here, q)
                q = cadd(q, row((f0, f1), j, k))
            put(j, cmul(gam, here))
        return carry

    lax.fori_loop(0, kc // KB, block, 0)


def inverse_z(chunk, part, s_ref, root, w_ref, fb, send, keep, u):
    me = lax.axis_index("py")
    _, ny, kc, nz = w_ref.shape
    w = send.shape[3]

    def block(i, carry):
        k = pl.ds(pl.multiple_of(i * KB, KB), KB)
        rows = own_rows(root, chunk * (kc // KB) + i, KB)
        lam = root[0, rows, :], root[1, rows, :]
        f = fb[0, k, :], fb[1, k, :]
        b = fb[2, k, :], fb[3, k, :]
        past = power(lam, ny)
        if part:
            f = cmul(past, f)
        else:
            b = cmul(past, b)
        for j in range(ny):
            f = cmul(lam, f)
            u[0, j], u[1, j] = cadd((w_ref[0, j, k, :], w_ref[1, j, k, :]), f)
        for j in reversed(range(ny)):
            b = cmul(lam, b)
            u[0, j], u[1, j] = cadd((u[0, j], u[1, j]), b)
        high, low = split(u[...].reshape(2 * ny * KB, nz))
        left = jnp.concatenate([high, low, high], axis=1)
        out = dot(left, stack(s_ref, 0))
        own, away = by_half(me, out[:, :w], out[:, w:])
        send[:, :, k, :] = away.reshape(2, ny, KB, w)
        keep[:, :, k, :] = own.reshape(2, ny, KB, w)
        return carry

    lax.fori_loop(0, kc // KB, block, 0)


def inverse_x(part, s_ref, *refs):
    *moved, src, speed, out, sums = refs
    number = len(moved) // 2
    me = lax.axis_index("py")
    _, nx, _, w = out.shape
    left = stack(s_ref, 1)
    for c in range(2):
        cols = []
        for y in range(YB):
            keep, recv = (jnp.concatenate([r[c, y] for r in rs], axis=0) for rs in (moved[:number], moved[number:]))
            high, low = split(jnp.concatenate(by_half(me, keep, recv), axis=0))
            cols.append(jnp.concatenate([high, low, high], axis=0))
        got = dot(left, jnp.concatenate(cols, axis=1))
        flat = out.at[c].reshape(nx * YB, w)
        for y in range(YB):
            flat[pl.ds(y, nx, stride=YB), :] = got[:, y * w : (y + 1) * w]
    here = pl.ds(part * YB, YB)
    damped = damping * wave_square

    def step(i, acc):
        s0, s1 = src[0, i, here, :], src[1, i, here, :]
        p0, p1 = out[0, i], out[1, i]
        c = speed[i, here, :]
        factor = wave_square - wave_square / (c * c)
        a0 = s0 + factor * p0 + damped * p1
        a1 = s1 + factor * p1 - damped * p0
        new = (
            s0 * s0 + s1 * s1,
            s0 * a0 + s1 * a1,
            s0 * a1 - s1 * a0,
            a0 * a0 + a1 * a1,
        )
        return tuple(x + y for x, y in zip(acc, new))

    zero = jnp.zeros((YB, w), f32)
    acc = lax.fori_loop(0, nx, step, (zero,) * 4, unroll=8)
    for i, a in enumerate(acc):
        sums[i : i + 1, :] = jnp.sum(a, axis=0, keepdims=True)


def finish(total, ps0, ps1, out_hbm, scaled, sems):
    sums = jnp.sum(jnp.sum(total[...], axis=0), axis=1, keepdims=True)
    square, re, im, size = (sums[i : i + 1] for i in range(4))
    beta2 = square + epsilon
    re, im, size = re / beta2, im / beta2, size / beta2
    den = size - (re * re + im * im) * (epsilon / beta2) + epsilon
    a, b = re / den, -im / den
    _, nx, _, w = ps0.shape
    a = jnp.broadcast_to(a, (YB, w))
    b = jnp.broadcast_to(b, (YB, w))
    copies = []
    for part, ps in enumerate((ps0, ps1)):
        for x in range(0, nx, XC):

            def step(i, carry, part=part, ps=ps):
                p0, p1 = ps[0, i], ps[1, i]
                scaled[part, 0, i] = a * p0 - b * p1
                scaled[part, 1, i] = a * p1 + b * p0
                return carry

            lax.fori_loop(x, x + XC, step, 0, unroll=8)
            copy = pltpu.make_async_copy(
                scaled.at[part, :, pl.ds(x, XC)],
                out_hbm.at[:, pl.ds(x, XC), pl.ds(part * YB, YB), :],
                sems.at[len(copies)],
            )
            copy.start()
            copies.append(copy)
    for copy in copies:
        copy.wait()


def params(mib, *dims):
    return pltpu.CompilerParams(dimension_semantics=dims or None, vmem_limit_bytes=mib * 2**20)


def whole(a):
    return pl.BlockSpec(a.shape, lambda *_: (0,) * a.ndim)


VM = pl.BlockSpec(memory_space=pltpu.VMEM)
ANY = pl.BlockSpec(memory_space=pl.ANY)


def cost(flops, moved):
    return pl.CostEstimate(flops=flops, bytes_accessed=moved, transcendentals=0)


def on_device(source, speed):
    _, nx, ny, w = source.shape
    cores, ring = lax.axis_size("py"), lax.axis_size("px")
    nz, nk = w * cores, nx // cores
    other = [(i, cores - 1 - i) for i in range(cores)]
    sds = lambda *shape: jax.ShapeDtypeStruct(shape, f32)

    table_x = jnp.asarray(np.stack(halves_of(sine_table(nx))))
    table_z = table_x if nz == nx else jnp.asarray(np.stack(halves_of(sine_table(nz))))
    root = jnp.asarray(root_tables(nx, nz))
    flops = 2 * 2 * nx * YB * w * nx * 3
    est = cost(flops, 4 * 2**20)

    kc = nk // CHUNKS
    plane, block, piece = sds(2, kc, nz), sds(2, YB, kc, nz), sds(2, ny, kc, w)
    parts = jax.ShapeDtypeStruct((2, ny // YB, 2 * nx, YB * w), bf16)
    moved, values = [], source
    for c in range(CHUNKS):
        first = c == 0
        send, keep, *left = pl.pallas_call(
            functools.partial(forward_x, c),
            in_specs=[VM] * 2,
            out_specs=[VM] * (2 + first),
            out_shape=[piece, piece] + [parts] * first,
            compiler_params=params(16),
            cost_estimate=est,
            name="forward_x",
        )(table_x, values)
        values = left[0] if first else values
        moved.append((keep, lax.ppermute(send, "py", other)))
    f, pq, sends, after = [], [], [], ()
    for c in range(CHUNKS):
        *got, carry, send, mark = pl.pallas_call(
            functools.partial(forward_z, c),
            in_specs=[VM] * (4 + len(after)),
            out_specs=[VM] * 5,
            out_shape=[block, block, sds(4, kc, nz), plane, sds(8, 128)],
            compiler_params=params(12),
            cost_estimate=est,
            name="forward_z",
        )(table_z, root, *moved[c], *after)
        after = (mark,)
        f.append(got)
        pq.append(carry)
        sends.append(send)

    def small(body, n_in, out, name):
        return pl.pallas_call(
            body,
            in_specs=[VM] * n_in,
            out_specs=VM if not isinstance(out, list) else [VM] * len(out),
            out_shape=out,
            compiler_params=params(4),
            cost_estimate=cost(2 * 10**6, 2**19),
            name=name,
        )

    def mirrored(pairs):
        return pairs + [(ring - 1 - a, ring - 1 - b) for a, b in pairs]

    pair = mirrored([(i, i + 1) for i in range(0, ring, 2)])
    quad = mirrored([(i, i + 2) for i in range(1, ring, 4)])
    steps = range(1, ring // 4 - 1)
    hops = [mirrored([(4 * m - 1, 4 * m + 3)]) for m in steps]
    down = mirrored([(i, i + 2) for i in range(3, ring - 2, 4)])
    local = [
        pl.pallas_call(
            functools.partial(local_solve, c),
            in_specs=[VM] * 3,
            out_specs=[VM, VM],
            out_shape=[block, block],
            compiler_params=params(8),
            cost_estimate=cost(flops // 8, 8 * 2**20),
            name="local_solve",
        )(root, *f[c])
        for c in range(CHUNKS)
    ]
    near = [lax.ppermute(s, "px", pair) for s in sends]
    now, after = [], ()
    for c, r in enumerate(near):
        got, mark = small(functools.partial(fold_pair, c, ny), 3 + len(after), [plane, sds(8, 128)], "fold")(
            root, pq[c], r, *after
        )
        now.append(got)
        after = (mark,)
    for level, (route, blocks) in enumerate([(quad, 2)] + [(hop, 4) for hop in hops] + [(down, 2)]):
        for c, s in enumerate(now):
            recv = lax.ppermute(s, "px", route)
            if level == 1:
                recv, local[c] = lax.optimization_barrier((recv, local[c]))
            now[c] = small(functools.partial(fold, c, [ny * blocks]), 3, plane, "fold")(root, s, recv)
    one = [lax.ppermute(s, "px", mirrored([(i, i + 1) for i in range(1, ring - 2, 2)])) for s in now]
    two = [lax.ppermute(s, "px", pair) for s in one]
    fb = [
        small(functools.partial(carries, c, ny), 5, sds(4, kc, nz), "carries")(root, pq[c], near[c], one[c], two[c])
        for c in range(CHUNKS)
    ]
    kept, sent = {}, {}
    half = sds(2, YB, kc, w)
    for h in range(2):
        for c in range(CHUNKS):
            send, kept[h, c] = pl.pallas_call(
                functools.partial(inverse_z, c, h),
                in_specs=[VM] * 4,
                out_specs=[VM, VM],
                out_shape=[half, half],
                scratch_shapes=[pltpu.VMEM((2, YB, KB, nz), f32)],
                compiler_params=params(12),
                cost_estimate=est,
                name="inverse_z",
            )(table_z, root, local[c][h], fb[c])
            sent[h, c] = lax.ppermute(send, "py", other)
    solved, sums = [], []
    for h in range(2):
        got, part = pl.pallas_call(
            functools.partial(inverse_x, h),
            in_specs=[VM] * (3 + 2 * CHUNKS),
            out_specs=[VM, VM],
            out_shape=[sds(2, nx, YB, w), sds(4, w)],
            compiler_params=params(16),
            cost_estimate=est,
            name="inverse_x",
        )(table_x, *(kept[h, c] for c in range(CHUNKS)), *(sent[h, c] for c in range(CHUNKS)), source, speed)
        solved.append(got)
        sums.append(part)
    sums = sums[0] + sums[1]
    sums = sums + lax.ppermute(sums, "py", other)
    every = lax.all_to_all(jnp.broadcast_to(sums[None], (ring, 4, w)), "px", 0, 0, tiled=True)
    return pl.pallas_call(
        finish,
        in_specs=[VM] * 3,
        out_specs=ANY,
        out_shape=sds(*source.shape),
        scratch_shapes=[pltpu.VMEM((2, 2, nx, YB, w), f32), pltpu.SemaphoreType.DMA((2 * nx // XC,))],
        compiler_params=params(16),
        cost_estimate=cost(10**7, 8 * 2**20),
        name="finish",
    )(every, *solved)


def solution(mesh):
    return jax.shard_map(
        on_device,
        mesh=mesh,
        in_specs=(P(None, "samples", "px", "py"), P("samples", "px", "py")),
        out_specs=P(None, "samples", "px", "py"),
        check_vma=False,
    )
```

```python
import functools
import numpy as np
import jax
import jax.numpy as jnp
from jax import lax
from jax.experimental import pallas as pl
from jax.experimental.pallas import tpu as pltpu
from jax.sharding import PartitionSpec as P

wave_square = 0.25
damping = 0.5
epsilon = 1e-06
f32 = jnp.float32
bf16 = jnp.bfloat16
YB = 8
KB = 32
XC = 32
CHUNKS = 2


def sine_table(length):
    k = np.arange(1, length + 1, dtype=np.float64)
    phases = np.mod(np.outer(k, k), 2 * (length + 1)) * (np.pi / (length + 1))
    return np.sqrt(2.0 / (length + 1)) * np.sin(phases)


def halves_of(table):
    table = table.astype(np.float32)
    high = table.astype(bf16)
    low = (table - high.astype(np.float32)).astype(bf16)
    return high, low


def eigen_line(length):
    k = np.arange(1, length + 1, dtype=np.float64)
    return 4.0 * np.sin(np.pi * k / (2.0 * (length + 1))) ** 2


def root_tables(nx, nz):
    near = eigen_line(nx)[:, None] + eigen_line(nz)[None, :] - wave_square + 1j * damping * wave_square
    spread = np.sqrt(near) * np.sqrt(near + 4.0)
    lam = 2.0 / (near + 2.0 + spread)
    gam = 1.0 / spread
    return np.stack([lam.real, lam.imag, gam.real, gam.imag]).astype(np.float32)


def cmul(a, b):
    return a[0] * b[0] - a[1] * b[1], a[0] * b[1] + a[1] * b[0]


def cadd(a, b):
    return a[0] + b[0], a[1] + b[1]


def split(v):
    high = v.astype(bf16)
    return high, (v - high.astype(f32)).astype(bf16)


def dot(a, b):
    return lax.dot_general(a, b, (((1,), (0,)), ((), ())), preferred_element_type=f32)


def stack(s_ref, axis):
    return jnp.concatenate([s_ref[0], s_ref[0], s_ref[1]], axis=axis)


def by_half(me, keep, recv):
    first = me == 0
    return jnp.where(first, keep, recv), jnp.where(first, recv, keep)


def forward_x_first(s_hbm, src_hbm, send, keep, parts, s_ref, values, sems):
    copies = [pltpu.make_async_copy(s_hbm, s_ref, sems.at[0])]
    for h in range(2):
        for c in range(2):
            rows = pl.ds(h * YB, YB)
            copies.append(pltpu.make_async_copy(src_hbm.at[c, :, rows, :], values.at[h, c], sems.at[1 + 2 * h + c]))
    for copy in copies:
        copy.start()
    forward_x(0, s_ref, values, send, keep, parts, copies=copies)


def forward_x(chunk, s_ref, values, send, keep, *parts, copies=()):
    me = lax.axis_index("py")
    _, ny, kc, w = send.shape
    nx = s_ref.shape[1]
    for h in range(ny // YB):
        for c in range(2):
            if parts:
                if copies:
                    copies[1 + 2 * h + c].wait()
                flat = values.at[h, c].reshape(nx * YB, w)
                cols = []
                for y in range(YB):
                    cols.append(jnp.concatenate(split(flat[pl.ds(y, nx, stride=YB), :]), axis=0))
                both = jnp.concatenate(cols, axis=1)
                parts[0][c, h] = both
            else:
                both = values[c, h]
            right = jnp.concatenate([both, both[:nx]], axis=0)
            if copies and not h and not c:
                copies[0].wait()
            left = []
            for half in (1 - me, me):
                rows = pl.ds(pl.multiple_of(half * (nx // 2) + chunk * kc, kc), kc)
                high, low = s_ref[0, rows, :], s_ref[1, rows, :]
                left.append(jnp.concatenate([high, high, low], axis=1))
            got = dot(jnp.concatenate(left, axis=0), right)
            for y in range(YB):
                send[c, h * YB + y] = got[:kc, y * w : (y + 1) * w]
                keep[c, h * YB + y] = got[kc:, y * w : (y + 1) * w]


def own_rows(root, block, kb):
    nk = root.shape[1] // 2
    return pl.ds(pl.multiple_of(lax.axis_index("py") * nk + block * kb, kb), kb)


def power(base, exponent):
    result = None
    while exponent:
        if exponent & 1:
            result = base if result is None else cmul(result, base)
        exponent >>= 1
        if exponent:
            base = cmul(base, base)
    return result


def forward_z(chunk, s_ref, root, keep, recv, *refs):
    *_, f0, f1, pq, send, done = refs
    done[...] = jnp.zeros_like(done)
    me = lax.axis_index("py")
    ring, place = lax.axis_size("px"), lax.axis_index("px")
    _, ny, kc, w = keep.shape
    nz = f0.shape[3]

    def block(i, carry):
        k = pl.ds(pl.multiple_of(i * KB, KB), KB)
        rows = own_rows(root, chunk * (kc // KB) + i, KB)
        lam = root[0, rows, :], root[1, rows, :]
        p, q = None, None
        for h, f in enumerate((f0, f1)):
            here = slice(h * YB, (h + 1) * YB)
            shape = 2 * YB * KB, w
            both = by_half(me, keep[:, here, k, :].reshape(shape), recv[:, here, k, :].reshape(shape))
            high, low = split(jnp.concatenate(both, axis=1))
            total = dot(jnp.concatenate([high, low, high], axis=1), stack(s_ref, 0))
            total = total.reshape(2, YB, KB, nz)
            f[:, :, k, :] = total
            row = [(total[0, j], total[1, j]) for j in range(YB)]
            p = row[0] if p is None else cadd(cmul(lam, p), row[0])
            part = row[YB - 1]
            for j in range(1, YB):
                p = cadd(cmul(lam, p), row[j])
                part = cadd(cmul(lam, part), row[YB - 1 - j])
            q = part if q is None else cadd(cmul(power(lam, h * YB), part), q)
        left, right = images(lam, 2 * ny, ring, place)
        edge = power(lam, ny + 1)
        p, q = (
            csub(p, cmul(cmul(left, edge), q)),
            csub(q, cmul(cmul(right, edge), p)),
        )
        even = place % 2 == 0
        for c in range(2):
            send[c, k, :] = jnp.where(even, p[c], q[c])
        for c, part in enumerate((*p, *q)):
            pq[c, k, :] = part
        return carry

    lax.fori_loop(0, kc // KB, block, 0)


def csub(a, b):
    return a[0] - b[0], a[1] - b[1]


def images(lam, step, ring, place):
    one, base = (jnp.ones_like(lam[0]), jnp.zeros_like(lam[0])), power(lam, step)
    found = [one, one]
    bit = 1
    while bit < ring:
        for i, number in enumerate((place, ring - 1 - place)):
            taken = (number // bit) % 2 == 1
            more = cmul(found[i], base)
            found[i] = tuple(jnp.where(taken, m, f) for m, f in zip(more, found[i]))
        base, bit = cmul(base, base), 2 * bit
    return found


def fold(chunk, exponents, root, now, *refs):
    *recv, out = refs
    kc = out.shape[1]
    rows = own_rows(root, chunk, kc)
    total = now[0], now[1]
    for exponent, r in zip(exponents, recv):
        far = power((root[0, rows, :], root[1, rows, :]), exponent)
        total = cadd(total, cmul(far, (r[0], r[1])))
    out[0], out[1] = total


def fold_pair(chunk, exponent, root, pq, recv, *refs):
    *_, out, done = refs
    done[...] = jnp.zeros_like(done)
    kc = out.shape[1]
    rows = own_rows(root, chunk, kc)
    far = power((root[0, rows, :], root[1, rows, :]), exponent)
    even = lax.axis_index("px") % 2 == 0
    now = tuple(jnp.where(even, pq[2 + c], pq[c]) for c in range(2))
    out[0], out[1] = cadd(now, cmul(far, (recv[0], recv[1])))


def carries(chunk, ny, root, pq, near, one, two, fb):
    kc, ring, place = fb.shape[1], lax.axis_size("px"), lax.axis_index("px")
    rows = own_rows(root, chunk, kc)
    lam = root[0, rows, :], root[1, rows, :]
    gam = root[2, rows, :], root[3, rows, :]
    block = power(lam, ny)
    direct = one[0], one[1]
    joined = cadd(cmul(block, (two[0], two[1])), (near[0], near[1]))
    even = place % 2 == 0
    f = tuple(jnp.where(even, a, b) for a, b in zip(direct, joined))
    b = tuple(jnp.where(even, b, a) for a, b in zip(direct, joined))
    p, q = (pq[0], pq[1]), (pq[2], pq[3])
    left, right = images(lam, 2 * ny, ring, place)
    whole = power(lam, 2 * (ny * ring + 1))
    det = 1.0 - whole[0], -whole[1]
    size = det[0] * det[0] + det[1] * det[1]
    scale = cmul(gam, (det[0] / size, -det[1] / size))
    f, b = (
        csub(f, cmul(cmul(left, lam), cadd(cmul(block, b), q))),
        csub(b, cmul(cmul(right, lam), cadd(cmul(block, f), p))),
    )
    fb[0], fb[1] = cmul(scale, f)
    fb[2], fb[3] = cmul(scale, b)


def local_solve(chunk, root, f0, f1, w0, w1):
    _, half, kc, _ = f0.shape
    ny = 2 * half

    def row(refs, j, k):
        ref = refs[j // half]
        return ref[0, j % half, k, :], ref[1, j % half, k, :]

    def block(i, carry):
        k = pl.ds(pl.multiple_of(i * KB, KB), KB)
        rows = own_rows(root, chunk * (kc // KB) + i, KB)
        lam = root[0, rows, :], root[1, rows, :]
        gam = root[2, rows, :], root[3, rows, :]

        def put(j, value):
            ref = (w0, w1)[j // half]
            ref[0, j % half, k, :], ref[1, j % half, k, :] = value

        p = None
        for j in range(ny):
            f = row((f0, f1), j, k)
            p = f if p is None else cadd(cmul(lam, p), f)
            put(j, p)
        q = None
        for j in reversed(range(ny)):
            here = row((w0, w1), j, k)
            if q is None:
                q = row((f0, f1), j, k)
            else:
                q = cmul(lam, q)
                here = cadd(here, q)
                q = cadd(q, row((f0, f1), j, k))
            put(j, cmul(gam, here))
        return carry

    lax.fori_loop(0, kc // KB, block, 0)


def inverse_z(chunk, part, s_ref, root, w_ref, fb, send, keep, u):
    me = lax.axis_index("py")
    _, ny, kc, nz = w_ref.shape
    w = send.shape[3]

    def block(i, carry):
        k = pl.ds(pl.multiple_of(i * KB, KB), KB)
        rows = own_rows(root, chunk * (kc // KB) + i, KB)
        lam = root[0, rows, :], root[1, rows, :]
        f = fb[0, k, :], fb[1, k, :]
        b = fb[2, k, :], fb[3, k, :]
        past = power(lam, ny)
        if part:
            f = cmul(past, f)
        else:
            b = cmul(past, b)
        for j in range(ny):
            f = cmul(lam, f)
            u[0, j], u[1, j] = cadd((w_ref[0, j, k, :], w_ref[1, j, k, :]), f)
        for j in reversed(range(ny)):
            b = cmul(lam, b)
            u[0, j], u[1, j] = cadd((u[0, j], u[1, j]), b)
        high, low = split(u[...].reshape(2 * ny * KB, nz))
        left = jnp.concatenate([high, low, high], axis=1)
        out = dot(left, stack(s_ref, 0))
        own, away = by_half(me, out[:, :w], out[:, w:])
        send[:, :, k, :] = away.reshape(2, ny, KB, w)
        keep[:, :, k, :] = own.reshape(2, ny, KB, w)
        return carry

    lax.fori_loop(0, kc // KB, block, 0)


def inverse_x(part, s_ref, *refs):
    *moved, src, speed, out, sums = refs
    number = len(moved) // 2
    me = lax.axis_index("py")
    _, nx, _, w = out.shape
    left = stack(s_ref, 1)
    for c in range(2):
        cols = []
        for y in range(YB):
            keep, recv = (jnp.concatenate([r[c, y] for r in rs], axis=0) for rs in (moved[:number], moved[number:]))
            high, low = split(jnp.concatenate(by_half(me, keep, recv), axis=0))
            cols.append(jnp.concatenate([high, low, high], axis=0))
        got = dot(left, jnp.concatenate(cols, axis=1))
        flat = out.at[c].reshape(nx * YB, w)
        for y in range(YB):
            flat[pl.ds(y, nx, stride=YB), :] = got[:, y * w : (y + 1) * w]
    here = pl.ds(part * YB, YB)
    damped = damping * wave_square

    def step(i, acc):
        s0, s1 = src[0, i, here, :], src[1, i, here, :]
        p0, p1 = out[0, i], out[1, i]
        c = speed[i, here, :]
        factor = wave_square - wave_square / (c * c)
        a0 = s0 + factor * p0 + damped * p1
        a1 = s1 + factor * p1 - damped * p0
        new = (
            s0 * s0 + s1 * s1,
            s0 * a0 + s1 * a1,
            s0 * a1 - s1 * a0,
            a0 * a0 + a1 * a1,
        )
        return tuple(x + y for x, y in zip(acc, new))

    zero = jnp.zeros((YB, w), f32)
    acc = lax.fori_loop(0, nx, step, (zero,) * 4, unroll=8)
    for i, a in enumerate(acc):
        sums[i : i + 1, :] = jnp.sum(a, axis=0, keepdims=True)


def finish(total, ps0, ps1, out_hbm, scaled, sems):
    sums = jnp.sum(jnp.sum(total[...], axis=0), axis=1, keepdims=True)
    square, re, im, size = (sums[i : i + 1] for i in range(4))
    beta2 = square + epsilon
    re, im, size = re / beta2, im / beta2, size / beta2
    den = size - (re * re + im * im) * (epsilon / beta2) + epsilon
    a, b = re / den, -im / den
    _, nx, _, w = ps0.shape
    a = jnp.broadcast_to(a, (YB, w))
    b = jnp.broadcast_to(b, (YB, w))
    copies = []
    for part, ps in enumerate((ps0, ps1)):
        for x in range(0, nx, XC):

            def step(i, carry, part=part, ps=ps):
                p0, p1 = ps[0, i], ps[1, i]
                scaled[part, 0, i] = a * p0 - b * p1
                scaled[part, 1, i] = a * p1 + b * p0
                return carry

            lax.fori_loop(x, x + XC, step, 0, unroll=8)
            copy = pltpu.make_async_copy(
                scaled.at[part, :, pl.ds(x, XC)],
                out_hbm.at[:, pl.ds(x, XC), pl.ds(part * YB, YB), :],
                sems.at[len(copies)],
            )
            copy.start()
            copies.append(copy)
    for copy in copies:
        copy.wait()


def params(mib, *dims):
    return pltpu.CompilerParams(dimension_semantics=dims or None, vmem_limit_bytes=mib * 2**20)


def whole(a):
    return pl.BlockSpec(a.shape, lambda *_: (0,) * a.ndim)


VM = pl.BlockSpec(memory_space=pltpu.VMEM)
ANY = pl.BlockSpec(memory_space=pl.ANY)


def cost(flops, moved):
    return pl.CostEstimate(flops=flops, bytes_accessed=moved, transcendentals=0)


def on_device(source, speed):
    _, nx, ny, w = source.shape
    cores, ring = lax.axis_size("py"), lax.axis_size("px")
    nz, nk = w * cores, nx // cores
    other = [(i, cores - 1 - i) for i in range(cores)]
    sds = lambda *shape: jax.ShapeDtypeStruct(shape, f32)

    table_x = jnp.asarray(np.stack(halves_of(sine_table(nx))))
    table_z = table_x if nz == nx else jnp.asarray(np.stack(halves_of(sine_table(nz))))
    root = jnp.asarray(root_tables(nx, nz))
    flops = 2 * 2 * nx * YB * w * nx * 3
    est = cost(flops, 4 * 2**20)

    kc = nk // CHUNKS
    plane, block, piece = sds(2, kc, nz), sds(2, YB, kc, nz), sds(2, ny, kc, w)
    parts = jax.ShapeDtypeStruct((2, ny // YB, 2 * nx, YB * w), bf16)
    moved, values = [], source
    for c in range(CHUNKS):
        first = c == 0
        send, keep, *left = pl.pallas_call(
            forward_x_first if first else functools.partial(forward_x, c),
            in_specs=[ANY if first else VM] * 2,
            out_specs=[VM] * (2 + first),
            out_shape=[piece, piece] + [parts] * first,
            scratch_shapes=[
                pltpu.VMEM(table_x.shape, bf16),
                pltpu.VMEM((2, 2, nx, YB, w), f32),
                pltpu.SemaphoreType.DMA((5,)),
            ]
            * first,
            compiler_params=params(45 if first else 16),
            cost_estimate=est,
            name="forward_x",
        )(table_x, values)
        values = left[0] if first else values
        moved.append((keep, lax.ppermute(send, "py", other)))
    f, pq, sends, after = [], [], [], ()
    for c in range(CHUNKS):
        *got, carry, send, mark = pl.pallas_call(
            functools.partial(forward_z, c),
            in_specs=[VM] * (4 + len(after)),
            out_specs=[VM] * 5,
            out_shape=[block, block, sds(4, kc, nz), plane, sds(8, 128)],
            compiler_params=params(12),
            cost_estimate=est,
            name="forward_z",
        )(table_z, root, *moved[c], *after)
        after = (mark,)
        f.append(got)
        pq.append(carry)
        sends.append(send)

    def small(body, n_in, out, name):
        return pl.pallas_call(
            body,
            in_specs=[VM] * n_in,
            out_specs=VM if not isinstance(out, list) else [VM] * len(out),
            out_shape=out,
            compiler_params=params(4),
            cost_estimate=cost(2 * 10**6, 2**19),
            name=name,
        )

    def mirrored(pairs):
        return pairs + [(ring - 1 - a, ring - 1 - b) for a, b in pairs]

    pair = mirrored([(i, i + 1) for i in range(0, ring, 2)])
    quad = mirrored([(i, i + 2) for i in range(1, ring, 4)])
    steps = range(1, ring // 4 - 1)
    hops = [mirrored([(4 * m - 1, 4 * m + 3)]) for m in steps]
    down = mirrored([(i, i + 2) for i in range(3, ring - 2, 4)])
    local = [
        pl.pallas_call(
            functools.partial(local_solve, c),
            in_specs=[VM] * 3,
            out_specs=[VM, VM],
            out_shape=[block, block],
            compiler_params=params(8),
            cost_estimate=cost(flops // 8, 8 * 2**20),
            name="local_solve",
        )(root, *f[c])
        for c in range(CHUNKS)
    ]
    near = [lax.ppermute(s, "px", pair) for s in sends]
    now, after = [], ()
    for c, r in enumerate(near):
        got, mark = small(functools.partial(fold_pair, c, ny), 3 + len(after), [plane, sds(8, 128)], "fold")(
            root, pq[c], r, *after
        )
        now.append(got)
        after = (mark,)
    for level, (route, blocks) in enumerate([(quad, 2)] + [(hop, 4) for hop in hops] + [(down, 2)]):
        for c, s in enumerate(now):
            recv = lax.ppermute(s, "px", route)
            if level == 1:
                recv, local[c] = lax.optimization_barrier((recv, local[c]))
            now[c] = small(functools.partial(fold, c, [ny * blocks]), 3, plane, "fold")(root, s, recv)
    one = [lax.ppermute(s, "px", mirrored([(i, i + 1) for i in range(1, ring - 2, 2)])) for s in now]
    two = [lax.ppermute(s, "px", pair) for s in one]
    fb = [
        small(functools.partial(carries, c, ny), 5, sds(4, kc, nz), "carries")(root, pq[c], near[c], one[c], two[c])
        for c in range(CHUNKS)
    ]
    kept, sent = {}, {}
    half = sds(2, YB, kc, w)
    for h in range(2):
        for c in range(CHUNKS):
            send, kept[h, c] = pl.pallas_call(
                functools.partial(inverse_z, c, h),
                in_specs=[VM] * 4,
                out_specs=[VM, VM],
                out_shape=[half, half],
                scratch_shapes=[pltpu.VMEM((2, YB, KB, nz), f32)],
                compiler_params=params(12),
                cost_estimate=est,
                name="inverse_z",
            )(table_z, root, local[c][h], fb[c])
            sent[h, c] = lax.ppermute(send, "py", other)
    solved, sums = [], []
    for h in range(2):
        got, part = pl.pallas_call(
            functools.partial(inverse_x, h),
            in_specs=[VM] * (3 + 2 * CHUNKS),
            out_specs=[VM, VM],
            out_shape=[sds(2, nx, YB, w), sds(4, w)],
            compiler_params=params(16),
            cost_estimate=est,
            name="inverse_x",
        )(table_x, *(kept[h, c] for c in range(CHUNKS)), *(sent[h, c] for c in range(CHUNKS)), source, speed)
        solved.append(got)
        sums.append(part)
    sums = sums[0] + sums[1]
    sums = sums + lax.ppermute(sums, "py", other)
    every = lax.all_to_all(jnp.broadcast_to(sums[None], (ring, 4, w)), "px", 0, 0, tiled=True)
    return pl.pallas_call(
        finish,
        in_specs=[VM] * 3,
        out_specs=ANY,
        out_shape=sds(*source.shape),
        scratch_shapes=[pltpu.VMEM((2, 2, nx, YB, w), f32), pltpu.SemaphoreType.DMA((2 * nx // XC,))],
        compiler_params=params(16),
        cost_estimate=cost(10**7, 8 * 2**20),
        name="finish",
    )(every, *solved)


def solution(mesh):
    return jax.shard_map(
        on_device,
        mesh=mesh,
        in_specs=(P(None, "samples", "px", "py"), P("samples", "px", "py")),
        out_specs=P(None, "samples", "px", "py"),
        check_vma=False,
    )
```

```python
import functools
import numpy as np
import jax
import jax.numpy as jnp
from jax import lax
from jax.experimental import pallas as pl
from jax.experimental.pallas import tpu as pltpu
from jax.sharding import PartitionSpec as P

wave_square = 0.25
damping = 0.5
epsilon = 1e-06
f32 = jnp.float32
bf16 = jnp.bfloat16
YB = 8
KB = 64
XC = 32
CHUNKS = 2


def sine_table(length):
    k = np.arange(1, length + 1, dtype=np.float64)
    phases = np.mod(np.outer(k, k), 2 * (length + 1)) * (np.pi / (length + 1))
    return np.sqrt(2.0 / (length + 1)) * np.sin(phases)


def halves_of(table):
    table = table.astype(np.float32)
    high = table.astype(bf16)
    low = (table - high.astype(np.float32)).astype(bf16)
    return high, low


def eigen_line(length):
    k = np.arange(1, length + 1, dtype=np.float64)
    return 4.0 * np.sin(np.pi * k / (2.0 * (length + 1))) ** 2


def root_tables(nx, nz):
    near = eigen_line(nx)[:, None] + eigen_line(nz)[None, :] - wave_square + 1j * damping * wave_square
    spread = np.sqrt(near) * np.sqrt(near + 4.0)
    lam = 2.0 / (near + 2.0 + spread)
    gam = 1.0 / spread
    return np.stack([lam.real, lam.imag, gam.real, gam.imag]).astype(np.float32)


def cmul(a, b):
    return a[0] * b[0] - a[1] * b[1], a[0] * b[1] + a[1] * b[0]


def cadd(a, b):
    return a[0] + b[0], a[1] + b[1]


def split(v):
    high = v.astype(bf16)
    return high, (v - high.astype(f32)).astype(bf16)


def dot(a, b):
    return lax.dot_general(a, b, (((1,), (0,)), ((), ())), preferred_element_type=f32)


def stack(s_ref, axis):
    return jnp.concatenate([s_ref[0], s_ref[0], s_ref[1]], axis=axis)


def by_half(me, keep, recv):
    first = me == 0
    return jnp.where(first, keep, recv), jnp.where(first, recv, keep)


def forward_x_first(s_hbm, src_hbm, send, keep, parts, s_ref, values, sems):
    copies = [pltpu.make_async_copy(s_hbm, s_ref, sems.at[0])]
    for h in range(2):
        for c in range(2):
            rows = pl.ds(h * YB, YB)
            copies.append(pltpu.make_async_copy(src_hbm.at[c, :, rows, :], values.at[h, c], sems.at[1 + 2 * h + c]))
    for copy in copies:
        copy.start()
    forward_x(0, s_ref, values, send, keep, parts, copies=copies)


def forward_x(chunk, s_ref, values, send, keep, *parts, copies=()):
    me = lax.axis_index("py")
    _, ny, kc, w = send.shape
    nx = s_ref.shape[1]
    for h in range(ny // YB):
        for c in range(2):
            if parts:
                if copies:
                    copies[1 + 2 * h + c].wait()
                flat = values.at[h, c].reshape(nx * YB, w)
                cols = []
                for y in range(YB):
                    cols.append(jnp.concatenate(split(flat[pl.ds(y, nx, stride=YB), :]), axis=0))
                both = jnp.concatenate(cols, axis=1)
                parts[0][c, h] = both
            else:
                both = values[c, h]
            right = jnp.concatenate([both, both[:nx]], axis=0)
            if copies and not h and not c:
                copies[0].wait()
            left = []
            for half in (1 - me, me):
                rows = pl.ds(pl.multiple_of(half * (nx // 2) + chunk * kc, kc), kc)
                high, low = s_ref[0, rows, :], s_ref[1, rows, :]
                left.append(jnp.concatenate([high, high, low], axis=1))
            got = dot(jnp.concatenate(left, axis=0), right)
            for y in range(YB):
                send[c, h * YB + y] = got[:kc, y * w : (y + 1) * w]
                keep[c, h * YB + y] = got[kc:, y * w : (y + 1) * w]


def own_rows(root, block, kb):
    nk = root.shape[1] // 2
    return pl.ds(pl.multiple_of(lax.axis_index("py") * nk + block * kb, kb), kb)


def power(base, exponent):
    result = None
    while exponent:
        if exponent & 1:
            result = base if result is None else cmul(result, base)
        exponent >>= 1
        if exponent:
            base = cmul(base, base)
    return result


def forward_z(chunk, s_ref, root, keep, recv, *refs):
    *_, f0, f1, pq, send, done = refs
    done[...] = jnp.zeros_like(done)
    me = lax.axis_index("py")
    ring, place = lax.axis_size("px"), lax.axis_index("px")
    _, ny, kc, w = keep.shape
    nz = f0.shape[3]

    def block(i, carry):
        k = pl.ds(pl.multiple_of(i * KB, KB), KB)
        rows = own_rows(root, chunk * (kc // KB) + i, KB)
        lam = root[0, rows, :], root[1, rows, :]
        p, q = None, None
        for h, f in enumerate((f0, f1)):
            here = slice(h * YB, (h + 1) * YB)
            shape = 2 * YB * KB, w
            both = by_half(me, keep[:, here, k, :].reshape(shape), recv[:, here, k, :].reshape(shape))
            high, low = split(jnp.concatenate(both, axis=1))
            total = dot(jnp.concatenate([high, low, high], axis=1), stack(s_ref, 0))
            total = total.reshape(2, YB, KB, nz)
            f[:, :, k, :] = total
            row = [(total[0, j], total[1, j]) for j in range(YB)]
            p = row[0] if p is None else cadd(cmul(lam, p), row[0])
            part = row[YB - 1]
            for j in range(1, YB):
                p = cadd(cmul(lam, p), row[j])
                part = cadd(cmul(lam, part), row[YB - 1 - j])
            q = part if q is None else cadd(cmul(power(lam, h * YB), part), q)
        left, right = images(lam, 2 * ny, ring, place)
        edge = power(lam, ny + 1)
        p, q = (
            csub(p, cmul(cmul(left, edge), q)),
            csub(q, cmul(cmul(right, edge), p)),
        )
        even = place % 2 == 0
        for c in range(2):
            send[c, k, :] = jnp.where(even, p[c], q[c])
        for c, part in enumerate((*p, *q)):
            pq[c, k, :] = part
        return carry

    lax.fori_loop(0, kc // KB, block, 0)


def csub(a, b):
    return a[0] - b[0], a[1] - b[1]


def images(lam, step, ring, place):
    one, base = (jnp.ones_like(lam[0]), jnp.zeros_like(lam[0])), power(lam, step)
    found = [one, one]
    bit = 1
    while bit < ring:
        for i, number in enumerate((place, ring - 1 - place)):
            taken = (number // bit) % 2 == 1
            more = cmul(found[i], base)
            found[i] = tuple(jnp.where(taken, m, f) for m, f in zip(more, found[i]))
        base, bit = cmul(base, base), 2 * bit
    return found


def fold(chunk, exponents, root, now, *refs):
    *recv, out = refs
    kc = out.shape[1]
    rows = own_rows(root, chunk, kc)
    total = now[0], now[1]
    for exponent, r in zip(exponents, recv):
        far = power((root[0, rows, :], root[1, rows, :]), exponent)
        total = cadd(total, cmul(far, (r[0], r[1])))
    out[0], out[1] = total


def fold_pair(chunk, exponent, root, pq, recv, *refs):
    *_, out, done = refs
    done[...] = jnp.zeros_like(done)
    kc = out.shape[1]
    rows = own_rows(root, chunk, kc)
    far = power((root[0, rows, :], root[1, rows, :]), exponent)
    even = lax.axis_index("px") % 2 == 0
    now = tuple(jnp.where(even, pq[2 + c], pq[c]) for c in range(2))
    out[0], out[1] = cadd(now, cmul(far, (recv[0], recv[1])))


def carries(chunk, ny, root, pq, near, one, two, fb):
    kc, ring, place = fb.shape[1], lax.axis_size("px"), lax.axis_index("px")
    rows = own_rows(root, chunk, kc)
    lam = root[0, rows, :], root[1, rows, :]
    gam = root[2, rows, :], root[3, rows, :]
    block = power(lam, ny)
    direct = one[0], one[1]
    joined = cadd(cmul(block, (two[0], two[1])), (near[0], near[1]))
    even = place % 2 == 0
    f = tuple(jnp.where(even, a, b) for a, b in zip(direct, joined))
    b = tuple(jnp.where(even, b, a) for a, b in zip(direct, joined))
    p, q = (pq[0], pq[1]), (pq[2], pq[3])
    left, right = images(lam, 2 * ny, ring, place)
    whole = power(lam, 2 * (ny * ring + 1))
    det = 1.0 - whole[0], -whole[1]
    size = det[0] * det[0] + det[1] * det[1]
    scale = cmul(gam, (det[0] / size, -det[1] / size))
    f, b = (
        csub(f, cmul(cmul(left, lam), cadd(cmul(block, b), q))),
        csub(b, cmul(cmul(right, lam), cadd(cmul(block, f), p))),
    )
    fb[0], fb[1] = cmul(scale, f)
    fb[2], fb[3] = cmul(scale, b)


def local_solve(chunk, root, f0, f1, w0, w1):
    _, half, kc, _ = f0.shape
    ny = 2 * half

    def row(refs, j, k):
        ref = refs[j // half]
        return ref[0, j % half, k, :], ref[1, j % half, k, :]

    def block(i, carry):
        k = pl.ds(pl.multiple_of(i * KB, KB), KB)
        rows = own_rows(root, chunk * (kc // KB) + i, KB)
        lam = root[0, rows, :], root[1, rows, :]
        gam = root[2, rows, :], root[3, rows, :]

        def put(j, value):
            ref = (w0, w1)[j // half]
            ref[0, j % half, k, :], ref[1, j % half, k, :] = value

        p = None
        for j in range(ny):
            f = row((f0, f1), j, k)
            p = f if p is None else cadd(cmul(lam, p), f)
            put(j, p)
        q = None
        for j in reversed(range(ny)):
            here = row((w0, w1), j, k)
            if q is None:
                q = row((f0, f1), j, k)
            else:
                q = cmul(lam, q)
                here = cadd(here, q)
                q = cadd(q, row((f0, f1), j, k))
            put(j, cmul(gam, here))
        return carry

    lax.fori_loop(0, kc // KB, block, 0)


def inverse_z(chunk, part, s_ref, root, w_ref, fb, send, keep, u):
    me = lax.axis_index("py")
    _, ny, kc, nz = w_ref.shape
    w = send.shape[3]

    def block(i, carry):
        k = pl.ds(pl.multiple_of(i * KB, KB), KB)
        rows = own_rows(root, chunk * (kc // KB) + i, KB)
        lam = root[0, rows, :], root[1, rows, :]
        f = fb[0, k, :], fb[1, k, :]
        b = fb[2, k, :], fb[3, k, :]
        past = power(lam, ny)
        if part:
            f = cmul(past, f)
        else:
            b = cmul(past, b)
        for j in range(ny):
            f = cmul(lam, f)
            u[0, j], u[1, j] = cadd((w_ref[0, j, k, :], w_ref[1, j, k, :]), f)
        for j in reversed(range(ny)):
            b = cmul(lam, b)
            u[0, j], u[1, j] = cadd((u[0, j], u[1, j]), b)
        high, low = split(u[...].reshape(2 * ny * KB, nz))
        left = jnp.concatenate([high, low, high], axis=1)
        out = dot(left, stack(s_ref, 0))
        own, away = by_half(me, out[:, :w], out[:, w:])
        send[:, :, k, :] = away.reshape(2, ny, KB, w)
        keep[:, :, k, :] = own.reshape(2, ny, KB, w)
        return carry

    lax.fori_loop(0, kc // KB, block, 0)


def inverse_x(part, s_ref, *refs):
    *moved, src, speed, out, sums = refs
    number = len(moved) // 2
    me = lax.axis_index("py")
    _, nx, _, w = out.shape
    left = stack(s_ref, 1)
    for c in range(2):
        cols = []
        for y in range(YB):
            keep, recv = (jnp.concatenate([r[c, y] for r in rs], axis=0) for rs in (moved[:number], moved[number:]))
            high, low = split(jnp.concatenate(by_half(me, keep, recv), axis=0))
            cols.append(jnp.concatenate([high, low, high], axis=0))
        got = dot(left, jnp.concatenate(cols, axis=1))
        flat = out.at[c].reshape(nx * YB, w)
        for y in range(YB):
            flat[pl.ds(y, nx, stride=YB), :] = got[:, y * w : (y + 1) * w]
    here = pl.ds(part * YB, YB)
    damped = damping * wave_square

    def step(i, acc):
        s0, s1 = src[0, i, here, :], src[1, i, here, :]
        p0, p1 = out[0, i], out[1, i]
        c = speed[i, here, :]
        factor = wave_square - wave_square / (c * c)
        a0 = s0 + factor * p0 + damped * p1
        a1 = s1 + factor * p1 - damped * p0
        new = (
            s0 * s0 + s1 * s1,
            s0 * a0 + s1 * a1,
            s0 * a1 - s1 * a0,
            a0 * a0 + a1 * a1,
        )
        return tuple(x + y for x, y in zip(acc, new))

    zero = jnp.zeros((YB, w), f32)
    acc = lax.fori_loop(0, nx, step, (zero,) * 4, unroll=8)
    for i, a in enumerate(acc):
        sums[i : i + 1, :] = jnp.sum(a, axis=0, keepdims=True)


def finish(total, ps0, ps1, out_hbm, scaled, sems):
    sums = jnp.sum(jnp.sum(total[...], axis=0), axis=1, keepdims=True)
    square, re, im, size = (sums[i : i + 1] for i in range(4))
    beta2 = square + epsilon
    re, im, size = re / beta2, im / beta2, size / beta2
    den = size - (re * re + im * im) * (epsilon / beta2) + epsilon
    a, b = re / den, -im / den
    _, nx, _, w = ps0.shape
    a = jnp.broadcast_to(a, (YB, w))
    b = jnp.broadcast_to(b, (YB, w))
    copies = []
    for part, ps in enumerate((ps0, ps1)):
        for x in range(0, nx, XC):

            def step(i, carry, part=part, ps=ps):
                p0, p1 = ps[0, i], ps[1, i]
                scaled[part, 0, i] = a * p0 - b * p1
                scaled[part, 1, i] = a * p1 + b * p0
                return carry

            lax.fori_loop(x, x + XC, step, 0, unroll=8)
            copy = pltpu.make_async_copy(
                scaled.at[part, :, pl.ds(x, XC)],
                out_hbm.at[:, pl.ds(x, XC), pl.ds(part * YB, YB), :],
                sems.at[len(copies)],
            )
            copy.start()
            copies.append(copy)
    for copy in copies:
        copy.wait()


def params(mib, *dims):
    return pltpu.CompilerParams(dimension_semantics=dims or None, vmem_limit_bytes=mib * 2**20)


def whole(a):
    return pl.BlockSpec(a.shape, lambda *_: (0,) * a.ndim)


VM = pl.BlockSpec(memory_space=pltpu.VMEM)
ANY = pl.BlockSpec(memory_space=pl.ANY)


def cost(flops, moved):
    return pl.CostEstimate(flops=flops, bytes_accessed=moved, transcendentals=0)


def on_device(source, speed):
    _, nx, ny, w = source.shape
    cores, ring = lax.axis_size("py"), lax.axis_size("px")
    nz, nk = w * cores, nx // cores
    other = [(i, cores - 1 - i) for i in range(cores)]
    sds = lambda *shape: jax.ShapeDtypeStruct(shape, f32)

    table_x = jnp.asarray(np.stack(halves_of(sine_table(nx))))
    table_z = table_x if nz == nx else jnp.asarray(np.stack(halves_of(sine_table(nz))))
    root = jnp.asarray(root_tables(nx, nz))
    flops = 2 * 2 * nx * YB * w * nx * 3
    est = cost(flops, 4 * 2**20)

    kc = nk // CHUNKS
    plane, block, piece = sds(2, kc, nz), sds(2, YB, kc, nz), sds(2, ny, kc, w)
    parts = jax.ShapeDtypeStruct((2, ny // YB, 2 * nx, YB * w), bf16)
    moved, values = [], source
    for c in range(CHUNKS):
        first = c == 0
        send, keep, *left = pl.pallas_call(
            forward_x_first if first else functools.partial(forward_x, c),
            in_specs=[ANY if first else VM] * 2,
            out_specs=[VM] * (2 + first),
            out_shape=[piece, piece] + [parts] * first,
            scratch_shapes=[
                pltpu.VMEM(table_x.shape, bf16),
                pltpu.VMEM((2, 2, nx, YB, w), f32),
                pltpu.SemaphoreType.DMA((5,)),
            ]
            * first,
            compiler_params=params(45 if first else 16),
            cost_estimate=est,
            name="forward_x",
        )(table_x, values)
        values = left[0] if first else values
        moved.append((keep, lax.ppermute(send, "py", other)))
    f, pq, sends, after = [], [], [], ()
    for c in range(CHUNKS):
        *got, carry, send, mark = pl.pallas_call(
            functools.partial(forward_z, c),
            in_specs=[VM] * (4 + len(after)),
            out_specs=[VM] * 5,
            out_shape=[block, block, sds(4, kc, nz), plane, sds(8, 128)],
            compiler_params=params(12),
            cost_estimate=est,
            name="forward_z",
        )(table_z, root, *moved[c], *after)
        after = (mark,)
        f.append(got)
        pq.append(carry)
        sends.append(send)

    def small(body, n_in, out, name):
        return pl.pallas_call(
            body,
            in_specs=[VM] * n_in,
            out_specs=VM if not isinstance(out, list) else [VM] * len(out),
            out_shape=out,
            compiler_params=params(4),
            cost_estimate=cost(2 * 10**6, 2**19),
            name=name,
        )

    def mirrored(pairs):
        return pairs + [(ring - 1 - a, ring - 1 - b) for a, b in pairs]

    pair = mirrored([(i, i + 1) for i in range(0, ring, 2)])
    quad = mirrored([(i, i + 2) for i in range(1, ring, 4)])
    steps = range(1, ring // 4 - 1)
    hops = [mirrored([(4 * m - 1, 4 * m + 3)]) for m in steps]
    down = mirrored([(i, i + 2) for i in range(3, ring - 2, 4)])
    local = [
        pl.pallas_call(
            functools.partial(local_solve, c),
            in_specs=[VM] * 3,
            out_specs=[VM, VM],
            out_shape=[block, block],
            compiler_params=params(8),
            cost_estimate=cost(flops // 8, 8 * 2**20),
            name="local_solve",
        )(root, *f[c])
        for c in range(CHUNKS)
    ]
    near = [lax.ppermute(s, "px", pair) for s in sends]
    now, after = [], ()
    for c, r in enumerate(near):
        got, mark = small(functools.partial(fold_pair, c, ny), 3 + len(after), [plane, sds(8, 128)], "fold")(
            root, pq[c], r, *after
        )
        now.append(got)
        after = (mark,)
    for level, (route, blocks) in enumerate([(quad, 2)] + [(hop, 4) for hop in hops] + [(down, 2)]):
        for c, s in enumerate(now):
            recv = lax.ppermute(s, "px", route)
            if level == 1:
                recv, local[c] = lax.optimization_barrier((recv, local[c]))
            now[c] = small(functools.partial(fold, c, [ny * blocks]), 3, plane, "fold")(root, s, recv)
    one = [lax.ppermute(s, "px", mirrored([(i, i + 1) for i in range(1, ring - 2, 2)])) for s in now]
    two = [lax.ppermute(s, "px", pair) for s in one]
    fb = [
        small(functools.partial(carries, c, ny), 5, sds(4, kc, nz), "carries")(root, pq[c], near[c], one[c], two[c])
        for c in range(CHUNKS)
    ]
    kept, sent = {}, {}
    half = sds(2, YB, kc, w)
    for h in range(2):
        for c in range(CHUNKS):
            send, kept[h, c] = pl.pallas_call(
                functools.partial(inverse_z, c, h),
                in_specs=[VM] * 4,
                out_specs=[VM, VM],
                out_shape=[half, half],
                scratch_shapes=[pltpu.VMEM((2, YB, KB, nz), f32)],
                compiler_params=params(12),
                cost_estimate=est,
                name="inverse_z",
            )(table_z, root, local[c][h], fb[c])
            sent[h, c] = lax.ppermute(send, "py", other)
    solved, sums = [], []
    for h in range(2):
        got, part = pl.pallas_call(
            functools.partial(inverse_x, h),
            in_specs=[VM] * (3 + 2 * CHUNKS),
            out_specs=[VM, VM],
            out_shape=[sds(2, nx, YB, w), sds(4, w)],
            compiler_params=params(16),
            cost_estimate=est,
            name="inverse_x",
        )(table_x, *(kept[h, c] for c in range(CHUNKS)), *(sent[h, c] for c in range(CHUNKS)), source, speed)
        solved.append(got)
        sums.append(part)
    sums = sums[0] + sums[1]
    sums = sums + lax.ppermute(sums, "py", other)
    every = lax.all_to_all(jnp.broadcast_to(sums[None], (ring, 4, w)), "px", 0, 0, tiled=True)
    return pl.pallas_call(
        finish,
        in_specs=[VM] * 3,
        out_specs=ANY,
        out_shape=sds(*source.shape),
        scratch_shapes=[pltpu.VMEM((2, 2, nx, YB, w), f32), pltpu.SemaphoreType.DMA((2 * nx // XC,))],
        compiler_params=params(16),
        cost_estimate=cost(10**7, 8 * 2**20),
        name="finish",
    )(every, *solved)


def solution(mesh):
    return jax.shard_map(
        on_device,
        mesh=mesh,
        in_specs=(P(None, "samples", "px", "py"), P("samples", "px", "py")),
        out_specs=P(None, "samples", "px", "py"),
        check_vma=False,
    )
```

```python
import functools
import numpy as np
import jax
import jax.numpy as jnp
from jax import lax
from jax.experimental import pallas as pl
from jax.experimental.pallas import tpu as pltpu
from jax.sharding import PartitionSpec as P

wave_square = 0.25
damping = 0.5
epsilon = 1e-06
f32 = jnp.float32
bf16 = jnp.bfloat16
YB = 8
KB = 64
XC = 16
CHUNKS = 2


def sine_table(length):
    k = np.arange(1, length + 1, dtype=np.float64)
    phases = np.mod(np.outer(k, k), 2 * (length + 1)) * (np.pi / (length + 1))
    return np.sqrt(2.0 / (length + 1)) * np.sin(phases)


def halves_of(table):
    table = table.astype(np.float32)
    high = table.astype(bf16)
    low = (table - high.astype(np.float32)).astype(bf16)
    return high, low


def eigen_line(length):
    k = np.arange(1, length + 1, dtype=np.float64)
    return 4.0 * np.sin(np.pi * k / (2.0 * (length + 1))) ** 2


def root_tables(nx, nz):
    near = eigen_line(nx)[:, None] + eigen_line(nz)[None, :] - wave_square + 1j * damping * wave_square
    spread = np.sqrt(near) * np.sqrt(near + 4.0)
    lam = 2.0 / (near + 2.0 + spread)
    gam = 1.0 / spread
    return np.stack([lam.real, lam.imag, gam.real, gam.imag]).astype(np.float32)


def cmul(a, b):
    return a[0] * b[0] - a[1] * b[1], a[0] * b[1] + a[1] * b[0]


def cadd(a, b):
    return a[0] + b[0], a[1] + b[1]


def split(v):
    high = v.astype(bf16)
    return high, (v - high.astype(f32)).astype(bf16)


def dot(a, b):
    return lax.dot_general(a, b, (((1,), (0,)), ((), ())), preferred_element_type=f32)


def stack(s_ref, axis):
    return jnp.concatenate([s_ref[0], s_ref[0], s_ref[1]], axis=axis)


def by_half(me, keep, recv):
    first = me == 0
    return jnp.where(first, keep, recv), jnp.where(first, recv, keep)


def forward_x_first(s_hbm, src_hbm, send, keep, parts, s_ref, values, sems):
    copies = [pltpu.make_async_copy(s_hbm, s_ref, sems.at[0])]
    for h in range(2):
        for c in range(2):
            rows = pl.ds(h * YB, YB)
            copies.append(pltpu.make_async_copy(src_hbm.at[c, :, rows, :], values.at[h, c], sems.at[1 + 2 * h + c]))
    for copy in copies:
        copy.start()
    forward_x(0, s_ref, values, send, keep, parts, copies=copies)


def forward_x(chunk, s_ref, values, send, keep, *parts, copies=()):
    me = lax.axis_index("py")
    _, ny, kc, w = send.shape
    nx = s_ref.shape[1]
    for h in range(ny // YB):
        for c in range(2):
            if parts:
                if copies:
                    copies[1 + 2 * h + c].wait()
                flat = values.at[h, c].reshape(nx * YB, w)
                cols = []
                for y in range(YB):
                    cols.append(jnp.concatenate(split(flat[pl.ds(y, nx, stride=YB), :]), axis=0))
                both = jnp.concatenate(cols, axis=1)
                parts[0][c, h] = both
            else:
                both = values[c, h]
            right = jnp.concatenate([both, both[:nx]], axis=0)
            if copies and not h and not c:
                copies[0].wait()
            left = []
            for half in (1 - me, me):
                rows = pl.ds(pl.multiple_of(half * (nx // 2) + chunk * kc, kc), kc)
                high, low = s_ref[0, rows, :], s_ref[1, rows, :]
                left.append(jnp.concatenate([high, high, low], axis=1))
            got = dot(jnp.concatenate(left, axis=0), right)
            for y in range(YB):
                send[c, h * YB + y] = got[:kc, y * w : (y + 1) * w]
                keep[c, h * YB + y] = got[kc:, y * w : (y + 1) * w]


def own_rows(root, block, kb):
    nk = root.shape[1] // 2
    return pl.ds(pl.multiple_of(lax.axis_index("py") * nk + block * kb, kb), kb)


def power(base, exponent):
    result = None
    while exponent:
        if exponent & 1:
            result = base if result is None else cmul(result, base)
        exponent >>= 1
        if exponent:
            base = cmul(base, base)
    return result


def forward_z(chunk, s_ref, root, keep, recv, *refs):
    *_, f0, f1, pq, send, done = refs
    done[...] = jnp.zeros_like(done)
    me = lax.axis_index("py")
    ring, place = lax.axis_size("px"), lax.axis_index("px")
    _, ny, kc, w = keep.shape
    nz = f0.shape[3]

    def block(i, carry):
        k = pl.ds(pl.multiple_of(i * KB, KB), KB)
        rows = own_rows(root, chunk * (kc // KB) + i, KB)
        lam = root[0, rows, :], root[1, rows, :]
        p, q = None, None
        for h, f in enumerate((f0, f1)):
            here = slice(h * YB, (h + 1) * YB)
            shape = 2 * YB * KB, w
            both = by_half(me, keep[:, here, k, :].reshape(shape), recv[:, here, k, :].reshape(shape))
            high, low = split(jnp.concatenate(both, axis=1))
            total = dot(jnp.concatenate([high, low, high], axis=1), stack(s_ref, 0))
            total = total.reshape(2, YB, KB, nz)
            f[:, :, k, :] = total
            row = [(total[0, j], total[1, j]) for j in range(YB)]
            p = row[0] if p is None else cadd(cmul(lam, p), row[0])
            part = row[YB - 1]
            for j in range(1, YB):
                p = cadd(cmul(lam, p), row[j])
                part = cadd(cmul(lam, part), row[YB - 1 - j])
            q = part if q is None else cadd(cmul(power(lam, h * YB), part), q)
        left, right = images(lam, 2 * ny, ring, place)
        edge = power(lam, ny + 1)
        p, q = (
            csub(p, cmul(cmul(left, edge), q)),
            csub(q, cmul(cmul(right, edge), p)),
        )
        even = place % 2 == 0
        for c in range(2):
            send[c, k, :] = jnp.where(even, p[c], q[c])
        for c, part in enumerate((*p, *q)):
            pq[c, k, :] = part
        return carry

    lax.fori_loop(0, kc // KB, block, 0)


def csub(a, b):
    return a[0] - b[0], a[1] - b[1]


def images(lam, step, ring, place):
    one, base = (jnp.ones_like(lam[0]), jnp.zeros_like(lam[0])), power(lam, step)
    found = [one, one]
    bit = 1
    while bit < ring:
        for i, number in enumerate((place, ring - 1 - place)):
            taken = (number // bit) % 2 == 1
            more = cmul(found[i], base)
            found[i] = tuple(jnp.where(taken, m, f) for m, f in zip(more, found[i]))
        base, bit = cmul(base, base), 2 * bit
    return found


def fold(chunk, exponents, root, now, *refs):
    *recv, out = refs
    kc = out.shape[1]
    rows = own_rows(root, chunk, kc)
    total = now[0], now[1]
    for exponent, r in zip(exponents, recv):
        far = power((root[0, rows, :], root[1, rows, :]), exponent)
        total = cadd(total, cmul(far, (r[0], r[1])))
    out[0], out[1] = total


def fold_pair(chunk, exponent, root, pq, recv, *refs):
    *_, out, done = refs
    done[...] = jnp.zeros_like(done)
    kc = out.shape[1]
    rows = own_rows(root, chunk, kc)
    far = power((root[0, rows, :], root[1, rows, :]), exponent)
    even = lax.axis_index("px") % 2 == 0
    now = tuple(jnp.where(even, pq[2 + c], pq[c]) for c in range(2))
    out[0], out[1] = cadd(now, cmul(far, (recv[0], recv[1])))


def carries(chunk, ny, root, pq, near, one, two, fb):
    kc, ring, place = fb.shape[1], lax.axis_size("px"), lax.axis_index("px")
    rows = own_rows(root, chunk, kc)
    lam = root[0, rows, :], root[1, rows, :]
    gam = root[2, rows, :], root[3, rows, :]
    block = power(lam, ny)
    direct = one[0], one[1]
    joined = cadd(cmul(block, (two[0], two[1])), (near[0], near[1]))
    even = place % 2 == 0
    f = tuple(jnp.where(even, a, b) for a, b in zip(direct, joined))
    b = tuple(jnp.where(even, b, a) for a, b in zip(direct, joined))
    p, q = (pq[0], pq[1]), (pq[2], pq[3])
    left, right = images(lam, 2 * ny, ring, place)
    whole = power(lam, 2 * (ny * ring + 1))
    det = 1.0 - whole[0], -whole[1]
    size = det[0] * det[0] + det[1] * det[1]
    scale = cmul(gam, (det[0] / size, -det[1] / size))
    f, b = (
        csub(f, cmul(cmul(left, lam), cadd(cmul(block, b), q))),
        csub(b, cmul(cmul(right, lam), cadd(cmul(block, f), p))),
    )
    fb[0], fb[1] = cmul(scale, f)
    fb[2], fb[3] = cmul(scale, b)


def local_solve(chunk, root, f0, f1, w0, w1):
    _, half, kc, _ = f0.shape
    ny = 2 * half

    def row(refs, j, k):
        ref = refs[j // half]
        return ref[0, j % half, k, :], ref[1, j % half, k, :]

    def block(i, carry):
        k = pl.ds(pl.multiple_of(i * KB, KB), KB)
        rows = own_rows(root, chunk * (kc // KB) + i, KB)
        lam = root[0, rows, :], root[1, rows, :]
        gam = root[2, rows, :], root[3, rows, :]

        def put(j, value):
            ref = (w0, w1)[j // half]
            ref[0, j % half, k, :], ref[1, j % half, k, :] = value

        p = None
        for j in range(ny):
            f = row((f0, f1), j, k)
            p = f if p is None else cadd(cmul(lam, p), f)
            put(j, p)
        q = None
        for j in reversed(range(ny)):
            here = row((w0, w1), j, k)
            if q is None:
                q = row((f0, f1), j, k)
            else:
                q = cmul(lam, q)
                here = cadd(here, q)
                q = cadd(q, row((f0, f1), j, k))
            put(j, cmul(gam, here))
        return carry

    lax.fori_loop(0, kc // KB, block, 0)


def inverse_z(chunk, part, s_ref, root, w_ref, fb, send, keep, u):
    me = lax.axis_index("py")
    _, ny, kc, nz = w_ref.shape
    w = send.shape[3]

    def block(i, carry):
        k = pl.ds(pl.multiple_of(i * KB, KB), KB)
        rows = own_rows(root, chunk * (kc // KB) + i, KB)
        lam = root[0, rows, :], root[1, rows, :]
        f = fb[0, k, :], fb[1, k, :]
        b = fb[2, k, :], fb[3, k, :]
        past = power(lam, ny)
        if part:
            f = cmul(past, f)
        else:
            b = cmul(past, b)
        for j in range(ny):
            f = cmul(lam, f)
            u[0, j], u[1, j] = cadd((w_ref[0, j, k, :], w_ref[1, j, k, :]), f)
        for j in reversed(range(ny)):
            b = cmul(lam, b)
            u[0, j], u[1, j] = cadd((u[0, j], u[1, j]), b)
        high, low = split(u[...].reshape(2 * ny * KB, nz))
        left = jnp.concatenate([high, low, high], axis=1)
        out = dot(left, stack(s_ref, 0))
        own, away = by_half(me, out[:, :w], out[:, w:])
        send[:, :, k, :] = away.reshape(2, ny, KB, w)
        keep[:, :, k, :] = own.reshape(2, ny, KB, w)
        return carry

    lax.fori_loop(0, kc // KB, block, 0)


def inverse_x(part, s_ref, *refs):
    *moved, src, speed, out, sums = refs
    number = len(moved) // 2
    me = lax.axis_index("py")
    _, nx, _, w = out.shape
    left = stack(s_ref, 1)
    for c in range(2):
        cols = []
        for y in range(YB):
            keep, recv = (jnp.concatenate([r[c, y] for r in rs], axis=0) for rs in (moved[:number], moved[number:]))
            high, low = split(jnp.concatenate(by_half(me, keep, recv), axis=0))
            cols.append(jnp.concatenate([high, low, high], axis=0))
        got = dot(left, jnp.concatenate(cols, axis=1))
        flat = out.at[c].reshape(nx * YB, w)
        for y in range(YB):
            flat[pl.ds(y, nx, stride=YB), :] = got[:, y * w : (y + 1) * w]
    here = pl.ds(part * YB, YB)
    damped = damping * wave_square

    def step(i, acc):
        s0, s1 = src[0, i, here, :], src[1, i, here, :]
        p0, p1 = out[0, i], out[1, i]
        c = speed[i, here, :]
        factor = wave_square - wave_square / (c * c)
        a0 = s0 + factor * p0 + damped * p1
        a1 = s1 + factor * p1 - damped * p0
        new = (
            s0 * s0 + s1 * s1,
            s0 * a0 + s1 * a1,
            s0 * a1 - s1 * a0,
            a0 * a0 + a1 * a1,
        )
        return tuple(x + y for x, y in zip(acc, new))

    zero = jnp.zeros((YB, w), f32)
    acc = lax.fori_loop(0, nx, step, (zero,) * 4, unroll=8)
    for i, a in enumerate(acc):
        sums[i : i + 1, :] = jnp.sum(a, axis=0, keepdims=True)


def finish(total, ps0, ps1, out_hbm, scaled, sems):
    sums = jnp.sum(jnp.sum(total[...], axis=0), axis=1, keepdims=True)
    square, re, im, size = (sums[i : i + 1] for i in range(4))
    beta2 = square + epsilon
    re, im, size = re / beta2, im / beta2, size / beta2
    den = size - (re * re + im * im) * (epsilon / beta2) + epsilon
    a, b = re / den, -im / den
    _, nx, _, w = ps0.shape
    a = jnp.broadcast_to(a, (YB, w))
    b = jnp.broadcast_to(b, (YB, w))
    copies = []
    for part, ps in enumerate((ps0, ps1)):
        for x in range(0, nx, XC):

            def step(i, carry, part=part, ps=ps):
                p0, p1 = ps[0, i], ps[1, i]
                scaled[part, 0, i] = a * p0 - b * p1
                scaled[part, 1, i] = a * p1 + b * p0
                return carry

            lax.fori_loop(x, x + XC, step, 0, unroll=8)
            copy = pltpu.make_async_copy(
                scaled.at[part, :, pl.ds(x, XC)],
                out_hbm.at[:, pl.ds(x, XC), pl.ds(part * YB, YB), :],
                sems.at[len(copies)],
            )
            copy.start()
            copies.append(copy)
    for copy in copies:
        copy.wait()


def params(mib, *dims):
    return pltpu.CompilerParams(dimension_semantics=dims or None, vmem_limit_bytes=mib * 2**20)


def whole(a):
    return pl.BlockSpec(a.shape, lambda *_: (0,) * a.ndim)


VM = pl.BlockSpec(memory_space=pltpu.VMEM)
ANY = pl.BlockSpec(memory_space=pl.ANY)


def cost(flops, moved):
    return pl.CostEstimate(flops=flops, bytes_accessed=moved, transcendentals=0)


def on_device(source, speed):
    _, nx, ny, w = source.shape
    cores, ring = lax.axis_size("py"), lax.axis_size("px")
    nz, nk = w * cores, nx // cores
    other = [(i, cores - 1 - i) for i in range(cores)]
    sds = lambda *shape: jax.ShapeDtypeStruct(shape, f32)

    table_x = jnp.asarray(np.stack(halves_of(sine_table(nx))))
    table_z = table_x if nz == nx else jnp.asarray(np.stack(halves_of(sine_table(nz))))
    root = jnp.asarray(root_tables(nx, nz))
    flops = 2 * 2 * nx * YB * w * nx * 3
    est = cost(flops, 4 * 2**20)

    kc = nk // CHUNKS
    plane, block, piece = sds(2, kc, nz), sds(2, YB, kc, nz), sds(2, ny, kc, w)
    parts = jax.ShapeDtypeStruct((2, ny // YB, 2 * nx, YB * w), bf16)
    moved, values = [], source
    for c in range(CHUNKS):
        first = c == 0
        send, keep, *left = pl.pallas_call(
            forward_x_first if first else functools.partial(forward_x, c),
            in_specs=[ANY if first else VM] * 2,
            out_specs=[VM] * (2 + first),
            out_shape=[piece, piece] + [parts] * first,
            scratch_shapes=[
                pltpu.VMEM(table_x.shape, bf16),
                pltpu.VMEM((2, 2, nx, YB, w), f32),
                pltpu.SemaphoreType.DMA((5,)),
            ]
            * first,
            compiler_params=params(45 if first else 16),
            cost_estimate=est,
            name="forward_x",
        )(table_x, values)
        values = left[0] if first else values
        moved.append((keep, lax.ppermute(send, "py", other)))
    f, pq, sends, after = [], [], [], ()
    for c in range(CHUNKS):
        *got, carry, send, mark = pl.pallas_call(
            functools.partial(forward_z, c),
            in_specs=[VM] * (4 + len(after)),
            out_specs=[VM] * 5,
            out_shape=[block, block, sds(4, kc, nz), plane, sds(8, 128)],
            compiler_params=params(12),
            cost_estimate=est,
            name="forward_z",
        )(table_z, root, *moved[c], *after)
        after = (mark,)
        f.append(got)
        pq.append(carry)
        sends.append(send)

    def small(body, n_in, out, name):
        return pl.pallas_call(
            body,
            in_specs=[VM] * n_in,
            out_specs=VM if not isinstance(out, list) else [VM] * len(out),
            out_shape=out,
            compiler_params=params(4),
            cost_estimate=cost(2 * 10**6, 2**19),
            name=name,
        )

    def mirrored(pairs):
        return pairs + [(ring - 1 - a, ring - 1 - b) for a, b in pairs]

    pair = mirrored([(i, i + 1) for i in range(0, ring, 2)])
    quad = mirrored([(i, i + 2) for i in range(1, ring, 4)])
    steps = range(1, ring // 4 - 1)
    hops = [mirrored([(4 * m - 1, 4 * m + 3)]) for m in steps]
    down = mirrored([(i, i + 2) for i in range(3, ring - 2, 4)])
    local = [
        pl.pallas_call(
            functools.partial(local_solve, c),
            in_specs=[VM] * 3,
            out_specs=[VM, VM],
            out_shape=[block, block],
            compiler_params=params(8),
            cost_estimate=cost(flops // 8, 8 * 2**20),
            name="local_solve",
        )(root, *f[c])
        for c in range(CHUNKS)
    ]
    near = [lax.ppermute(s, "px", pair) for s in sends]
    now, after = [], ()
    for c, r in enumerate(near):
        got, mark = small(functools.partial(fold_pair, c, ny), 3 + len(after), [plane, sds(8, 128)], "fold")(
            root, pq[c], r, *after
        )
        now.append(got)
        after = (mark,)
    for level, (route, blocks) in enumerate([(quad, 2)] + [(hop, 4) for hop in hops] + [(down, 2)]):
        for c, s in enumerate(now):
            recv = lax.ppermute(s, "px", route)
            if level == 1:
                recv, local[c] = lax.optimization_barrier((recv, local[c]))
            now[c] = small(functools.partial(fold, c, [ny * blocks]), 3, plane, "fold")(root, s, recv)
    one = [lax.ppermute(s, "px", mirrored([(i, i + 1) for i in range(1, ring - 2, 2)])) for s in now]
    two = [lax.ppermute(s, "px", pair) for s in one]
    fb = [
        small(functools.partial(carries, c, ny), 5, sds(4, kc, nz), "carries")(root, pq[c], near[c], one[c], two[c])
        for c in range(CHUNKS)
    ]
    kept, sent = {}, {}
    half = sds(2, YB, kc, w)
    for h in range(2):
        for c in range(CHUNKS):
            send, kept[h, c] = pl.pallas_call(
                functools.partial(inverse_z, c, h),
                in_specs=[VM] * 4,
                out_specs=[VM, VM],
                out_shape=[half, half],
                scratch_shapes=[pltpu.VMEM((2, YB, KB, nz), f32)],
                compiler_params=params(12),
                cost_estimate=est,
                name="inverse_z",
            )(table_z, root, local[c][h], fb[c])
            sent[h, c] = lax.ppermute(send, "py", other)
    solved, sums = [], []
    for h in range(2):
        got, part = pl.pallas_call(
            functools.partial(inverse_x, h),
            in_specs=[VM] * (3 + 2 * CHUNKS),
            out_specs=[VM, VM],
            out_shape=[sds(2, nx, YB, w), sds(4, w)],
            compiler_params=params(16),
            cost_estimate=est,
            name="inverse_x",
        )(table_x, *(kept[h, c] for c in range(CHUNKS)), *(sent[h, c] for c in range(CHUNKS)), source, speed)
        solved.append(got)
        sums.append(part)
    sums = sums[0] + sums[1]
    sums = sums + lax.ppermute(sums, "py", other)
    every = lax.all_to_all(jnp.broadcast_to(sums[None], (ring, 4, w)), "px", 0, 0, tiled=True)
    return pl.pallas_call(
        finish,
        in_specs=[VM] * 3,
        out_specs=ANY,
        out_shape=sds(*source.shape),
        scratch_shapes=[pltpu.VMEM((2, 2, nx, YB, w), f32), pltpu.SemaphoreType.DMA((2 * nx // XC,))],
        compiler_params=params(16),
        cost_estimate=cost(10**7, 8 * 2**20),
        name="finish",
    )(every, *solved)


def solution(mesh):
    return jax.shard_map(
        on_device,
        mesh=mesh,
        in_specs=(P(None, "samples", "px", "py"), P("samples", "px", "py")),
        out_specs=P(None, "samples", "px", "py"),
        check_vma=False,
    )
```
